32 devices in a mesh: fsdp: 8 (over z, y), seq: 4 (over x, core).
Axes of the slice: x: 2, y: 2, z: 4, core: 2. Of those that a mesh axis runs over, the one named last changes fastest.
Arguments:
- tokens: bfloat16 [16384, 1024], P(('fsdp', 'seq')), may hold values from -6 to 6
- cotangent: bfloat16 [16384, 1024], P(('fsdp', 'seq')), may hold values from -6 to 6
- seq_lengths: int32 [8, 4], P('fsdp'), may hold values from 1 to 1024, 2048 in all within a row
- stream_order: int32 [8, 2048], P('fsdp'), may hold values from 0 to 2047, each once within a row
- first_gain: bfloat16 [1024], P('fsdp'), may hold values from 0.099609375 to 1.8984375
- first_shift: bfloat16 [1024], P('fsdp'), may hold values from -2 to 2
- qkv_weight: bfloat16 [1024, 3072], P('fsdp'), may hold values from -0.1875 to 0.1875
- query_bias: bfloat16 [1024], P('fsdp'), may hold values from -3 to 3
- value_bias: bfloat16 [1024], P('fsdp'), may hold values from -3 to 3
- out_weight: bfloat16 [1024, 1024], P('fsdp'), may hold values from -0.5 to 0.5
- out_bias: bfloat16 [1024], P('fsdp'), may hold values from -2 to 2
- second_gain: bfloat16 [1024], P('fsdp'), may hold values from 0.099609375 to 1.8984375
- second_shift: bfloat16 [1024], P('fsdp'), may hold values from -2 to 2
- up_weight: bfloat16 [1024, 4096], P('fsdp'), may hold values from -0.1875 to 0.1875
- up_bias: bfloat16 [4096], P('fsdp'), may hold values from -3 to 3
- down_weight: bfloat16 [4096, 1024], P('fsdp'), may hold values from -0.09375 to 0.09375
- down_bias: bfloat16 [1024], P('fsdp'), may hold values from -2 to 2
Outputs:
- output: bfloat16 [16384, 1024], P(('fsdp', 'seq'))
- tokens_grad: float32 [16384, 1024], P(('fsdp', 'seq'))
- first_gain_grad: float32 [1024], P('fsdp')
- first_shift_grad: float32 [1024], P('fsdp')
- qkv_weight_grad: float32 [1024, 3072], P('fsdp')
- query_bias_grad: float32 [1024], P('fsdp')
- value_bias_grad: float32 [1024], P('fsdp')
- out_weight_grad: float32 [1024, 1024], P('fsdp')
- out_bias_grad: float32 [1024], P('fsdp')
- second_gain_grad: float32 [1024], P('fsdp')
- second_shift_grad: float32 [1024], P('fsdp')
- up_weight_grad: float32 [1024, 4096], P('fsdp')
- up_bias_grad: float32 [4096], P('fsdp')
- down_weight_grad: float32 [4096, 1024], P('fsdp')
- down_bias_grad: float32 [1024], P('fsdp')
The draws below stay inside these ranges and needn't reach their ends.
Inputs may be any that keep to these rules, and one draw needn't show every extreme that they name: `seq_lengths`: row g lists the lengths of group g's sequences, which sum to 2048; the longest is exactly 1024. `stream_order`: each row is a permutation of the group's stream positions.
All inputs are finite; a program needn't handle non-finite values.
Results may differ from the reference program's by a relative error of at most 0.018.
Values may be sent and summed in bfloat16 or wider, within the bound.
A program may use at most 192 MiB of HBM per device.

```python
import math
import jax
import jax.numpy as jnp
import numpy as np
from jax import lax

D = 1024
HEADS = 16
HEAD_DIM = 64
FF = 4096
GROUP_TOK = 2048
GROUPS = 8
TOKENS = 16384
MOST_LEN = 1024
SEQ_SLOTS = 4


def block_levels(rng, dims, shards, least, top_value):
    loudness = 1.0
    for dim, parts in shards:
        heights = jax.random.uniform(jax.random.fold_in(jax.random.fold_in(rng, 6), dim), (parts,), jnp.float32, least / len(shards), top_value / len(shards))
        loudness = loudness * jnp.repeat(jnp.exp(heights), dims[dim] // parts).reshape((-1,) + (1,) * (len(dims) - 1 - dim))
    return loudness


def split_up(count, total, bound, slope):
    weights = [(1 << 20) // math.isqrt(standing ** slope) + 1 for standing in range(2, count + 1)]
    rest, holding = total - bound - (count - 1), [1] * (count - 1)
    while rest > 0:
        candidates = [i for i in range(count - 1) if holding[i] < bound]
        mass, remaining = sum([weights[i] for i in candidates]), rest
        for i in candidates:
            addition = min(bound - holding[i], max(1, remaining * weights[i] // mass), rest)
            holding[i] = holding[i] + addition
            rest = rest - addition
    return np.array([bound] + holding)


def ragged_sizes(own_key, count, total, reach, slope):
    if count == 2:
        one = jax.random.randint(own_key, (), max(1, total - reach), min(reach, total - 1) + 1)
        return jnp.stack([one, total - one])
    lengths = jnp.asarray(split_up(count, total, reach, slope), jnp.int32)
    couples = (count - 1) // 2
    giver, sink = lengths[1:1 + 2 * couples:2], lengths[2:2 + 2 * couples:2]
    room = jnp.minimum(giver - 1, reach - sink)
    passed = jax.random.randint(jax.random.fold_in(own_key, 1), (couples,), 0, 1 << 20) % (room + 1)
    lengths = lengths.at[1:1 + 2 * couples:2].set(giver - passed).at[2:2 + 2 * couples:2].set(sink + passed)
    return lengths[jax.random.permutation(jax.random.fold_in(own_key, 2), count)]


def centred(key, extent, scale, most, pieces=(), kind=jnp.bfloat16):
    drawn = jax.random.normal(key, extent, jnp.float32) * scale
    if len(pieces) > 0:
        drawn = block_levels(key, extent, pieces, -0.22, 0.18) * drawn
    return jnp.clip(drawn, min=-most, max=most).astype(kind)


def setup_inputs(seed: int = 0) -> dict:
    keys = jax.random.split(jax.random.key(seed), 18)
    tokens = centred(keys[0], (TOKENS, D), 1.0, 6.0, ((0, 32),))
    cotangent = centred(keys[1], (TOKENS, D), 1.0, 6.0, ((0, 32),))
    seq_lengths = jax.vmap(lambda own: ragged_sizes(own, SEQ_SLOTS, GROUP_TOK, MOST_LEN, 2))(jax.random.split(keys[2], GROUPS)).reshape((GROUPS, SEQ_SLOTS)).astype(jnp.int32)
    stream_order = jax.vmap(lambda own: jax.random.permutation(own, GROUP_TOK))(jax.random.split(keys[3], GROUPS)).reshape((GROUPS, GROUP_TOK)).astype(jnp.int32)
    first_gain = jnp.clip(1.0 + 0.18 * jax.random.normal(keys[4], (D,), jnp.float32), 0.099609375, 1.8984375).astype(jnp.bfloat16)
    first_shift = centred(keys[5], (D,), 0.3, 2.0, ((0, 8),))
    qkv_weight = centred(keys[6], (D, 3 * D), D ** -0.5, 0.1875, ((0, 8),))
    query_bias = centred(keys[7], (D,), 0.5, 3.0, ((0, 8),))
    value_bias = centred(keys[8], (D,), 0.5, 3.0, ((0, 8),))
    out_weight = centred(keys[9], (D, D), (D // 8) ** -0.5, 0.5, ((0, 8),))
    out_bias = centred(keys[10], (D,), 0.3, 2.0, ((0, 8),))
    second_gain = jnp.clip(1.0 + 0.18 * jax.random.normal(keys[11], (D,), jnp.float32), 0.099609375, 1.8984375).astype(jnp.bfloat16)
    second_shift = centred(keys[12], (D,), 0.3, 2.0, ((0, 8),))
    up_weight = centred(keys[13], (D, FF), D ** -0.5, 0.1875, ((0, 8),))
    up_bias = centred(keys[14], (FF,), 0.5, 3.0, ((0, 8),))
    down_weight = centred(keys[15], (FF, D), FF ** -0.5, 0.09375, ((0, 8),))
    down_bias = centred(keys[16], (D,), 0.3, 2.0, ((0, 8),))
    return {"tokens": tokens, "cotangent": cotangent, "seq_lengths": seq_lengths, "stream_order": stream_order, "first_gain": first_gain, "first_shift": first_shift, "qkv_weight": qkv_weight, "query_bias": query_bias, "value_bias": value_bias, "out_weight": out_weight, "out_bias": out_bias, "second_gain": second_gain, "second_shift": second_shift, "up_weight": up_weight, "up_bias": up_bias, "down_weight": down_weight, "down_bias": down_bias}


@jax.custom_vjp
def low(v):
    return lax.optimization_barrier(v.astype(jnp.bfloat16)).astype(jnp.float32)

@jax.custom_vjp
def low_back(v):
    return v

def low_keep(v):
    return (low(v), None)

def low_pass(kept, grad):
    return (grad,)

def back_keep(v):
    return (v, None)

def back_low(kept, grad):
    return (low(grad),)
low.defvjp(low_keep, low_pass)
low_back.defvjp(back_keep, back_low)

def layer_norm(values, norm_gain, norm_shift):
    average = lax.optimization_barrier(jnp.mean(values, axis=-1, keepdims=True))
    centered = values - average
    variance = lax.optimization_barrier(jnp.mean(centered * centered, axis=-1, keepdims=True))
    return centered * lax.rsqrt(variance + 1e-05) * norm_gain + norm_shift

def matmul(left, right):
    return jnp.dot(left, right, precision=lax.Precision.HIGHEST)

def attend_block(queries, query_pos, query_seg, key_rows, value_rows, key_pos, key_seg, slopes):
    scores = jnp.einsum('qhd,khd->hqk', queries, key_rows, precision=lax.Precision.HIGHEST) * (1.0 / math.sqrt(HEAD_DIM))
    distance = (query_pos[:, None] - key_pos[None, :]).astype(jnp.float32)
    scores = scores - slopes[:, None, None] * distance[None]
    allowed = (query_seg[:, None] == key_seg[None, :]) & (key_pos[None, :] <= query_pos[:, None])
    scores = low_back(jnp.where(allowed[None], scores, -1e+30))
    attn_probs = low(jax.nn.softmax(scores, axis=-1))
    return jnp.einsum('hqk,khd->qhd', attn_probs, value_rows, precision=lax.Precision.HIGHEST)

def reference(tokens, cotangent, seq_lengths, stream_order, first_gain, first_shift, qkv_weight, query_bias, value_bias, out_weight, out_bias, second_gain, second_shift, up_weight, up_bias, down_weight, down_bias):
    positions = stream_order.astype(jnp.int32)
    seq_ends = jnp.cumsum(seq_lengths.astype(jnp.int32), axis=1).astype(jnp.int32)
    segments = lax.optimization_barrier(jnp.sum((positions[:, :, None] >= seq_ends[:, None, :]).astype(jnp.int32), axis=2)).astype(jnp.int32)
    slopes = jnp.exp2(-(jnp.arange(HEADS).astype(jnp.float32) + 1.0) * (8.0 / HEADS))
    block_rows = min(512, GROUP_TOK)
    block_count = GROUP_TOK // block_rows
    checked = jax.checkpoint(attend_block)

    def attend_group(group_data):
        queries, key_rows, value_rows, group_pos, group_seg = group_data

        def one_block(member):
            return checked(member[0], member[1], member[2], key_rows, value_rows, group_pos, group_seg, slopes)
        result = lax.map(one_block, (queries.reshape(block_count, block_rows, HEADS, HEAD_DIM), group_pos.reshape(block_count, block_rows), group_seg.reshape(block_count, block_rows)))
        return result.reshape(GROUP_TOK, HEADS, HEAD_DIM)

    def forward(inputs, params):
        gain_one, shift_one, w_qkv, bias_query, bias_value, w_out, bias_out, gain_two, shift_two, w_up, bias_up, w_down, bias_down = params
        normed = low(layer_norm(inputs, gain_one, shift_one))
        projected = matmul(normed, w_qkv)
        queries = low(low_back(projected[:, :D] + bias_query))
        key_rows = low(low_back(projected[:, D:2 * D]))
        value_rows = low(low_back(projected[:, 2 * D:] + bias_value))
        head_shape = (GROUPS, GROUP_TOK, HEADS, HEAD_DIM)
        context = lax.map(attend_group, (queries.reshape(head_shape), key_rows.reshape(head_shape), value_rows.reshape(head_shape), positions, segments))
        context = low(low_back(context.reshape(TOKENS, D)))
        residual = inputs + low_back(matmul(context, w_out) + bias_out)
        hidden = low(layer_norm(residual, gain_two, shift_two))
        pre_act = low_back(matmul(hidden, w_up) + bias_up)
        activated = low(jax.nn.gelu(pre_act, approximate=True))
        return residual + low_back(matmul(activated, w_down) + bias_down)
    params = tuple((member.astype(jnp.float32) for member in (first_gain, first_shift, qkv_weight, query_bias, value_bias, out_weight, out_bias, second_gain, second_shift, up_weight, up_bias, down_weight, down_bias)))
    result, pullback = jax.vjp(forward, tokens.astype(jnp.float32), params)
    input_grad, gradients = pullback(cotangent.astype(jnp.float32))
    return (result.astype(jnp.bfloat16), input_grad, gradients[0], gradients[1], gradients[2], gradients[3], gradients[4], gradients[5], gradients[6], gradients[7], gradients[8], gradients[9], gradients[10], gradients[11], gradients[12])
```

```python
import functools
import math

import jax
import jax.numpy as jnp
from jax import lax
from jax.experimental import pallas as pl
from jax.experimental.pallas import tpu as pltpu
from jax.sharding import PartitionSpec as P

HEADS = 16
HEAD_DIM = 64
LANES = 128
BF = jnp.bfloat16
F32 = jnp.float32
MASKED = -1e30


def swap(value, axis, size, bit):
    return lax.ppermute(value, axis, [(i, i ^ bit) for i in range(size)])


def gather_pieces(value, axis, size):
    pieces = {0: value}
    bit = size // 2
    while bit:
        for r in sorted(pieces):
            pieces[r | bit] = swap(pieces[r], axis, size, bit)
        bit //= 2
    return [pieces[r] for r in range(size)]


def scatter_sum(pieces, axis, size, last=F32):
    held = dict(enumerate(pieces))
    bit = 1
    while bit < size:
        for r in sorted(held):
            if r & bit:
                arrived = swap(held.pop(r), axis, size, bit)
                total = held[r ^ bit].astype(F32) + arrived.astype(F32)
                held[r ^ bit] = total.astype(last if bit * 2 == size else arrived.dtype)
        bit *= 2
    return held[0]


def vmem():
    return pl.BlockSpec(memory_space=pltpu.VMEM)


def smem():
    return pl.BlockSpec(memory_space=pltpu.SMEM)


def whole_call(body, outs, me, *arrays):
    return pl.pallas_call(
        body,
        out_shape=outs,
        in_specs=[smem()] + [vmem()] * len(arrays),
        out_specs=jax.tree.map(lambda _: vmem(), outs),
    )(me.reshape(1).astype(jnp.int32), *arrays)


def place_rows(pieces, me):
    count, (rows, cols) = len(pieces), pieces[0].shape

    def body(me_ref, *refs):
        for r in range(count):
            spot = pl.multiple_of((me_ref[0] ^ r) * rows, rows)
            refs[-1][pl.ds(spot, rows), :] = refs[r][...]

    return whole_call(
        body, jax.ShapeDtypeStruct((count * rows, cols), pieces[0].dtype), me, *pieces
    )


def place_cols(pieces, me):
    count, (rows, cols) = len(pieces), pieces[0].shape

    def body(me_ref, *refs):
        for r in range(count):
            spot = pl.multiple_of((me_ref[0] ^ r) * cols, cols)
            refs[-1][:, pl.ds(spot, cols)] = refs[r][...]

    return whole_call(
        body, jax.ShapeDtypeStruct((rows, count * cols), pieces[0].dtype), me, *pieces
    )


def take_rows(value, count, me):
    rows, cols = value.shape[0] // count, value.shape[1]

    def body(me_ref, src, *outs):
        for r in range(count):
            spot = pl.multiple_of((me_ref[0] ^ r) * rows, rows)
            outs[r][...] = src[pl.ds(spot, rows), :]

    return whole_call(
        body, [jax.ShapeDtypeStruct((rows, cols), value.dtype)] * count, me, value
    )


def take_cols(value, count, me):
    rows, cols = value.shape[0], value.shape[1] // count

    def body(me_ref, src, *outs):
        for r in range(count):
            spot = pl.multiple_of((me_ref[0] ^ r) * cols, cols)
            outs[r][...] = src[:, pl.ds(spot, cols)]

    return whole_call(
        body, [jax.ShapeDtypeStruct((rows, cols), value.dtype)] * count, me, value
    )


def in_order(pieces, me):
    return jnp.stack(pieces)[jnp.arange(len(pieces)) ^ me]


def pair_mask(shape, head):
    lane = lax.broadcasted_iota(jnp.int32, shape, 1)
    return (lane >= head * HEAD_DIM) & (lane < (head + 1) * HEAD_DIM)


def dot_nt(a, b):
    return lax.dot_general(a, b, (((1,), (1,)), ((), ())), preferred_element_type=F32)


def dot_nn(a, b):
    return lax.dot_general(a, b, (((1,), (0,)), ((), ())), preferred_element_type=F32)


def dot_tn(a, b):
    return lax.dot_general(a, b, (((0,), (0,)), ((), ())), preferred_element_type=F32)


def distance_tile(start_row, row_at, key_at, keys, rows):
    key = lax.broadcasted_iota(jnp.int32, (keys, rows), 0) + key_at
    row = lax.broadcasted_iota(jnp.int32, (keys, rows), 1) + row_at
    allowed = (key <= row) & (key >= start_row)
    return jnp.where(allowed, (key - row).astype(F32), MASKED)


def attend_body(block, low_ref, slope_ref, start_ref, q_ref, k_ref, v_ref, o_ref, lse_ref, m_ref, l_ref, acc_ref):
    pair, step = pl.program_id(0), pl.program_id(1)
    m_ref[...] = jnp.full_like(m_ref, -3e38)
    l_ref[...] = jnp.zeros_like(l_ref)
    acc_ref[...] = jnp.zeros_like(acc_ref)
    queries = q_ref[...]
    start_row = start_ref[...]
    heads = [jnp.where(pair_mask(queries.shape, h), queries, 0).astype(BF) for h in range(2)]

    def tile(j, _):
        at = pl.multiple_of(j * block, block)
        keys = k_ref[pl.ds(at, block), :]
        values = v_ref[pl.ds(at, block), :]
        dist = distance_tile(start_row, step * block, at, block, block)
        for h in range(2):
            scores = dot_nt(keys, heads[h]) + slope_ref[pair * 2 + h] * dist
            old = m_ref[h : h + 1, :]
            new = jnp.maximum(old, jnp.max(scores, axis=0, keepdims=True))
            shrink = jnp.exp(old - new)
            weight = jnp.exp(scores - new)
            m_ref[h : h + 1, :] = new
            l_ref[h : h + 1, :] = l_ref[h : h + 1, :] * shrink + jnp.sum(
                weight, axis=0, keepdims=True
            )
            acc_ref[h] = acc_ref[h] * shrink + dot_tn(values, weight.astype(BF))
        return 0

    lax.fori_loop(low_ref[step], step + 1, tile, 0)
    top = acc_ref[0] / l_ref[0:1, :]
    bottom = acc_ref[1] / l_ref[1:2, :]
    row = lax.broadcasted_iota(jnp.int32, top.shape, 0)
    o_ref[...] = jnp.where(row < HEAD_DIM, top, bottom).T.astype(BF)
    lse_ref[...] = (m_ref[...] + jnp.log(l_ref[...])).reshape(lse_ref.shape)


def attend(qkv, low, slopes, start, block):
    rows, width = qkv.shape[0], qkv.shape[1] // 3
    pairs = width // LANES
    return pl.pallas_call(
        functools.partial(attend_body, block),
        out_shape=(
            jax.ShapeDtypeStruct((rows, width), BF),
            jax.ShapeDtypeStruct((pairs, 2, rows), F32),
        ),
        grid=(pairs, rows // block),
        in_specs=[
            smem(),
            smem(),
            pl.BlockSpec((1, block), lambda p, i: (0, i)),
            pl.BlockSpec((block, LANES), lambda p, i: (i, p)),
            pl.BlockSpec((rows, LANES), lambda p, i: (0, pairs + p)),
            pl.BlockSpec((rows, LANES), lambda p, i: (0, 2 * pairs + p)),
        ],
        out_specs=(
            pl.BlockSpec((block, LANES), lambda p, i: (i, p)),
            pl.BlockSpec((1, 2, block), lambda p, i: (p, 0, i)),
        ),
        scratch_shapes=[
            pltpu.VMEM((2, block), F32),
            pltpu.VMEM((2, block), F32),
            pltpu.VMEM((2, LANES, block), F32),
        ],
        cost_estimate=pl.CostEstimate(
            flops=rows * rows * width, bytes_accessed=10 * rows * width, transcendentals=rows * rows
        ),
        name="attend",
    )(low, slopes, start, qkv, qkv, qkv)


def attend_back_body(
    block, low_ref, slope_ref, start_ref, lse_ref, q_ref, k_ref, v_ref, o_ref, g_ref, dq_ref, dk_ref, dv_ref, dq_acc, dk_acc, dv_acc
):
    pair, step = pl.program_id(0), pl.program_id(1)

    @pl.when(step == 0)
    def _():
        dk_acc[...] = jnp.zeros_like(dk_acc)
        dv_acc[...] = jnp.zeros_like(dv_acc)

    dq_acc[...] = jnp.zeros_like(dq_acc)
    queries, grads = q_ref[...], g_ref[...]
    start_row = start_ref[...]
    product = (o_ref[...].astype(F32) * grads.astype(F32)).T
    dots = [
        jnp.sum(product[h * HEAD_DIM : (h + 1) * HEAD_DIM], axis=0, keepdims=True) for h in range(2)
    ]
    masks = [pair_mask(queries.shape, h) for h in range(2)]
    q_heads = [jnp.where(m, queries, 0).astype(BF) for m in masks]
    g_heads = [jnp.where(m, grads, 0).astype(BF) for m in masks]

    def tile(j, _):
        at = pl.multiple_of(j * block, block)
        keys = k_ref[pl.ds(at, block), :]
        values = v_ref[pl.ds(at, block), :]
        dist = distance_tile(start_row, step * block, at, block, block)
        dk = dk_acc[pl.ds(at, block), :]
        dv = dv_acc[pl.ds(at, block), :]
        dq = dq_acc[...]
        for h in range(2):
            scores = dot_nt(keys, q_heads[h]) + slope_ref[pair * 2 + h] * dist
            prob = jnp.exp(scores - lse_ref[0, h : h + 1, :])
            dprob = dot_nt(values, g_heads[h])
            dscore = (prob * (dprob - dots[h])).astype(BF)
            dv += dot_nn(prob.astype(BF), g_heads[h])
            dk += dot_nn(dscore, q_heads[h])
            key_head = jnp.where(masks[h], keys, 0).astype(BF)
            dq += dot_tn(key_head, dscore)
        dk_acc[pl.ds(at, block), :] = dk
        dv_acc[pl.ds(at, block), :] = dv
        dq_acc[...] = dq
        return 0

    lax.fori_loop(low_ref[step], step + 1, tile, 0)
    dq_ref[...] = (dq_acc[...].T * (1.0 / math.sqrt(HEAD_DIM))).astype(BF)

    @pl.when(step == pl.num_programs(1) - 1)
    def _():
        dk_ref[...] = dk_acc[...].astype(BF)
        dv_ref[...] = dv_acc[...].astype(BF)


def attend_back(qkv, out, grad, lse, low, slopes, start, block):
    rows, width = qkv.shape[0], qkv.shape[1] // 3
    pairs = width // LANES
    return pl.pallas_call(
        functools.partial(attend_back_body, block),
        out_shape=[jax.ShapeDtypeStruct((rows, width), BF)] * 3,
        grid=(pairs, rows // block),
        in_specs=[
            smem(),
            smem(),
            pl.BlockSpec((1, block), lambda p, i: (0, i)),
            pl.BlockSpec((1, 2, block), lambda p, i: (p, 0, i)),
            pl.BlockSpec((block, LANES), lambda p, i: (i, p)),
            pl.BlockSpec((rows, LANES), lambda p, i: (0, pairs + p)),
            pl.BlockSpec((rows, LANES), lambda p, i: (0, 2 * pairs + p)),
            pl.BlockSpec((block, LANES), lambda p, i: (i, p)),
            pl.BlockSpec((block, LANES), lambda p, i: (i, p)),
        ],
        out_specs=[
            pl.BlockSpec((block, LANES), lambda p, i: (i, p)),
            pl.BlockSpec((rows, LANES), lambda p, i: (0, p)),
            pl.BlockSpec((rows, LANES), lambda p, i: (0, p)),
        ],
        scratch_shapes=[
            pltpu.VMEM((LANES, block), F32),
            pltpu.VMEM((rows, LANES), F32),
            pltpu.VMEM((rows, LANES), F32),
        ],
        cost_estimate=pl.CostEstimate(
            flops=3 * rows * rows * width, bytes_accessed=20 * rows * width, transcendentals=rows * rows
        ),
        name="attend_back",
    )(low, slopes, start, lse, qkv, qkv, qkv, out, grad)


def normalize(values):
    average = jnp.mean(values, axis=-1, keepdims=True)
    centered = values - average
    variance = jnp.mean(centered * centered, axis=-1, keepdims=True)
    scale = lax.rsqrt(variance + 1e-05)
    return centered * scale, scale


def norm_back(grad, gain, normed, scale):
    e = grad * gain
    return scale * (
        e
        - jnp.mean(e, axis=-1, keepdims=True)
        - normed * jnp.mean(e * normed, axis=-1, keepdims=True)
    )


def gelu_and_slope(v):
    c = math.sqrt(2 / math.pi)
    t = jnp.tanh(c * (v + 0.044715 * v * v * v))
    slope = 0.5 * (1 + t) + 0.5 * v * (1 - t * t) * c * (1 + 3 * 0.044715 * v * v)
    return 0.5 * v * (1 + t), slope


def mm(a, b):
    return jnp.dot(a, b, preferred_element_type=F32)


def mm_nt(a, b):
    return lax.dot_general(a, b, (((1,), (1,)), ((), ())), preferred_element_type=F32)


def mm_tn(a, b):
    return lax.dot_general(a, b, (((0,), (0,)), ((), ())), preferred_element_type=F32)


def shards(
    nf,
    ns,
    tokens,
    cotangent,
    seq_lengths,
    stream_order,
    first_gain,
    first_shift,
    qkv_weight,
    query_bias,
    value_bias,
    out_weight,
    out_bias,
    second_gain,
    second_shift,
    up_weight,
    up_bias,
    down_weight,
    down_bias,
):
    f, s = lax.axis_index("fsdp"), lax.axis_index("seq")
    toks, width = tokens.shape
    group = toks * ns
    dl, hl = width // nf, width // ns
    ff = up_weight.shape[1]
    ffl = ff // nf
    q = ffl // ns

    vectors = jnp.concatenate(
        [first_gain, first_shift, query_bias, value_bias, out_bias, second_gain, second_shift, down_bias, up_bias]
    ).reshape(-1, dl)
    vec_pieces = gather_pieces(vectors, "fsdp", nf)
    qkv_shard = jnp.concatenate(
        [lax.dynamic_slice(qkv_weight, (0, k * width + s * hl), (dl, hl)) for k in range(3)], axis=1
    )
    qkv_pieces = gather_pieces(qkv_shard, "fsdp", nf)
    x_pieces = gather_pieces(tokens, "seq", ns)
    out_pieces = gather_pieces(
        lax.dynamic_slice(out_weight, (0, s * hl), (dl, hl)), "fsdp", nf
    )
    up_shard = lax.dynamic_index_in_dim(
        up_weight.reshape(dl, nf, ns, q), s, 2, keepdims=False
    ).reshape(dl, nf * q)
    up_pieces = gather_pieces(up_shard, "fsdp", nf)
    down_pieces = gather_pieces(
        lax.dynamic_slice(down_weight, (s * q, 0), (q, width)), "fsdp", nf
    )
    ct_pieces = gather_pieces(cotangent, "seq", ns)

    vecs = in_order(vec_pieces, f).astype(F32)
    full = vecs[:, :8].transpose(1, 0, 2).reshape(8, width)
    gain_one, shift_one, bias_query, bias_value, bias_out, gain_two, shift_two, bias_down = full
    bias_up = lax.dynamic_index_in_dim(vecs[:, 8:].reshape(nf, ns, q), s, 1, keepdims=False)
    bias_up = bias_up.reshape(nf * q)
    bias_qkv = jnp.concatenate(
        [
            lax.dynamic_slice(bias_query, (s * hl,), (hl,)),
            jnp.zeros((hl,), F32),
            lax.dynamic_slice(bias_value, (s * hl,), (hl,)),
        ]
    )
    query_scale = jnp.where(jnp.arange(3 * hl) < hl, 1.0 / math.sqrt(HEAD_DIM), 1.0)

    positions = in_order(list(stream_order[0].reshape(ns, toks)), s).reshape(group)
    ends = jnp.cumsum(seq_lengths[0])
    line = jnp.arange(group)
    start = jnp.max(jnp.where(ends[None, :] <= line[:, None], ends[None, :], 0), axis=1)
    block = min(256, group)
    low = (start[::block] // block).astype(jnp.int32)
    start_row = start.astype(jnp.int32)[None, :]
    heads_here = hl // HEAD_DIM
    slopes = jnp.exp2(
        -(s * heads_here + 1 + jnp.arange(heads_here)).astype(F32) * (8.0 / HEADS)
    )
    to_sorted = (positions[None, :] == line[:, None]).astype(BF)

    x_all = jnp.concatenate(x_pieces, axis=0)
    n_all, _ = normalize(x_all.astype(F32))
    a_all = (n_all * gain_one + shift_one).astype(BF)
    qkv_full = place_rows(qkv_pieces, f)
    qkv = ((mm(a_all, qkv_full) + bias_qkv).astype(BF).astype(F32) * query_scale).astype(BF)
    qkv_sorted = mm(to_sorted, qkv).astype(BF)
    o_sorted, lse = attend(qkv_sorted, low, slopes, start_row, block)
    context_heads = mm_tn(to_sorted, o_sorted).astype(BF)
    context_pieces = [context_heads[j * toks : (j + 1) * toks] for j in range(ns)]
    context = place_cols(
        [context_pieces[0]] + [swap(context_pieces[j], "seq", ns, j) for j in range(1, ns)], s
    )

    out_cols = place_rows(out_pieces, f)
    out_full = place_cols(gather_pieces(out_cols, "seq", ns), s)
    x_own = tokens.astype(F32)
    residual = x_own + mm(context, out_full) + bias_out
    n_two, scale_two = normalize(residual)
    m_low = (n_two * gain_two + shift_two).astype(BF)
    m_all = jnp.concatenate(gather_pieces(m_low, "seq", ns), axis=0)
    up_full = place_rows(up_pieces, f)
    down_full = place_rows(down_pieces, f)
    ct_all = jnp.concatenate(ct_pieces, axis=0)
    activated, slope = gelu_and_slope(mm(m_all, up_full) + bias_up)
    act = activated.astype(BF)
    slope = slope.astype(BF)
    d_pre = (mm_nt(ct_all, down_full) * slope.astype(F32)).astype(BF)
    d_m_part = mm_nt(d_pre, up_full).astype(BF)
    d_m = scatter_sum([d_m_part[j * toks : (j + 1) * toks] for j in range(ns)], "seq", ns)
    total = mm(act, down_full).astype(BF)
    total = scatter_sum([total[j * toks : (j + 1) * toks] for j in range(ns)], "seq", ns)
    output = (residual + total + bias_down).astype(BF)
    grad_down = scatter_sum(take_rows(mm_tn(act, ct_all).astype(BF), nf, f), "fsdp", nf, BF)
    grad_up = scatter_sum(take_rows(mm_tn(m_all, d_pre).astype(BF), nf, f), "fsdp", nf, BF)
    grad_up_bias = jnp.sum(d_pre, axis=0, dtype=F32)

    ct_own = cotangent.astype(F32)
    grad_down_bias = jnp.sum(ct_own, axis=0)
    grad_gain_two = jnp.sum(d_m * n_two, axis=0)
    grad_shift_two = jnp.sum(d_m, axis=0)
    d_res = ct_own + norm_back(d_m, gain_two, n_two, scale_two)
    d_att = d_res.astype(BF)
    grad_out_bias = jnp.sum(d_att, axis=0, dtype=F32)
    d_context_pieces = take_cols(mm_nt(d_att, out_full).astype(BF), ns, s)
    d_context = jnp.concatenate(
        [d_context_pieces[0]] + [swap(d_context_pieces[j], "seq", ns, j) for j in range(1, ns)],
        axis=0,
    )
    d_o_sorted = mm(to_sorted, d_context).astype(BF)
    grad_out = scatter_sum(take_cols(mm_tn(context, d_att).astype(BF), ns, s), "seq", ns, BF)
    grad_out = scatter_sum(take_rows(grad_out, nf, f), "fsdp", nf, BF)

    d_qkv_sorted = jnp.concatenate(
        attend_back(qkv_sorted, o_sorted, d_o_sorted, lse, low, slopes, start_row, block), axis=1
    )
    d_qkv = mm_tn(to_sorted, d_qkv_sorted).astype(BF)
    d_a_part = mm_nt(d_qkv, qkv_full)
    d_a_low = d_a_part.astype(BF)
    d_a = scatter_sum([d_a_low[j * toks : (j + 1) * toks] for j in range(ns)], "seq", ns)
    grad_qkv = scatter_sum(take_rows(mm_tn(a_all, d_qkv).astype(BF), nf, f), "fsdp", nf, BF)
    grad_bias_qkv = jnp.sum(d_qkv, axis=0, dtype=F32)
    grad_gain_one = jnp.sum(d_a_part * n_all, axis=0)
    grad_shift_one = jnp.sum(d_a_part, axis=0)
    n_own, scale_own = normalize(x_own)
    tokens_grad = d_res + norm_back(d_a, gain_one, n_own, scale_own)

    def spread(part):
        return lax.dynamic_update_slice(jnp.zeros((width,), F32), part, (s * hl,))

    vec_rows = jnp.stack(
        [
            grad_gain_one,
            grad_shift_one,
            spread(grad_bias_qkv[:hl]),
            spread(grad_bias_qkv[2 * hl :]),
            grad_out_bias,
            grad_gain_two,
            grad_shift_two,
            grad_down_bias,
        ]
    )
    vec_rows = vec_rows.reshape(8, nf, dl).transpose(1, 0, 2)
    up_rows = lax.dynamic_update_slice(
        jnp.zeros((nf, ns, q), F32), grad_up_bias.reshape(nf, 1, q), (0, s, 0)
    ).reshape(nf, -1, dl)
    vec_rows = jnp.concatenate([vec_rows, up_rows], axis=1)[jnp.arange(nf) ^ f]
    vec_sum = scatter_sum([vec_rows[r] for r in range(nf)], "fsdp", nf)
    bit = ns // 2
    while bit:
        vec_sum = vec_sum + swap(vec_sum, "seq", ns, bit)
        bit //= 2

    def everywhere(part):
        return in_order(gather_pieces(part, "seq", ns), s).astype(F32)

    down_all = everywhere(grad_down).reshape(ffl, width)
    up_all = everywhere(grad_up).reshape(ns, dl, nf, q).transpose(1, 2, 0, 3).reshape(dl, ff)
    out_all = everywhere(grad_out).transpose(1, 0, 2).reshape(dl, width)
    qkv_all = everywhere(grad_qkv).reshape(ns, dl, 3, hl).transpose(1, 2, 0, 3).reshape(dl, 3 * width)
    return (
        output,
        tokens_grad,
        vec_sum[0],
        vec_sum[1],
        qkv_all,
        vec_sum[2],
        vec_sum[3],
        out_all,
        vec_sum[4],
        vec_sum[5],
        vec_sum[6],
        up_all,
        vec_sum[8:].reshape(ffl),
        down_all,
        vec_sum[7],
    )


def solution(mesh):
    rows, cols, vec = P(("fsdp", "seq"), None), P("fsdp", None), P("fsdp")
    return jax.shard_map(
        functools.partial(shards, mesh.shape["fsdp"], mesh.shape["seq"]),
        mesh=mesh,
        in_specs=(rows, rows, cols, cols, vec, vec, cols, vec, vec, cols, vec, vec, vec, cols, vec, cols, vec),
        out_specs=(rows, rows, vec, vec, cols, vec, vec, cols, vec, vec, vec, cols, vec, cols, vec),
        check_vma=False,
    )
```

```python
import functools
import math

import jax
import jax.numpy as jnp
from jax import lax
from jax.experimental import pallas as pl
from jax.experimental.pallas import tpu as pltpu
from jax.sharding import PartitionSpec as P

HEADS = 16
HEAD_DIM = 64
LANES = 128
BF = jnp.bfloat16
F32 = jnp.float32
MASKED = -1e30


def swap(value, axis, size, bit):
    return lax.ppermute(value, axis, [(i, i ^ bit) for i in range(size)])


def falling(size):
    bits = []
    while size > 1:
        size //= 2
        bits.append(size)
    return tuple(bits)


def order_of(bits):
    order = [0]
    for bit in bits:
        order = order + [k ^ bit for k in order]
    return order


def gather_rows(value, axis, size, bits):
    for bit in bits:
        value = jnp.concatenate([value, swap(value, axis, size, bit)], axis=0)
    return value


def scatter_rows(keep, send, axis, size, bits, last=F32):
    for k, bit in enumerate(bits):
        arrived = swap(send, axis, size, bit)
        if k == len(bits) - 1:
            return (keep.astype(F32) + arrived.astype(F32)).astype(last)
        half = keep.shape[0] // 2
        send = (keep[half:].astype(F32) + arrived[half:].astype(F32)).astype(keep.dtype)
        keep = (keep[:half].astype(F32) + arrived[:half].astype(F32)).astype(keep.dtype)


def vmem():
    return pl.BlockSpec(memory_space=pltpu.VMEM)


def smem():
    return pl.BlockSpec(memory_space=pltpu.SMEM)


def whole_call(body, outs, me, *arrays):
    return pl.pallas_call(
        body,
        out_shape=outs,
        in_specs=[smem()] + [vmem()] * len(arrays),
        out_specs=jax.tree.map(lambda _: vmem(), outs),
    )(me.reshape(1).astype(jnp.int32), *arrays)


def place_weights(parts, orders, rows, extra, me):
    count, cols = len(orders[0]), parts[0].shape[1]

    def body(me_ref, *refs):
        *sources, main, more = refs
        for p, (source, order) in enumerate(zip(sources, orders)):
            at = slice(p * cols, (p + 1) * cols)
            for k, r in enumerate(order):
                base = k * (rows + extra)
                here = me_ref[0] ^ r
                main[pl.ds(pl.multiple_of(here * rows, rows), rows), at] = source[base : base + rows, :]
                more[pl.ds(pl.multiple_of(here * extra, extra), extra), at] = source[
                    base + rows : base + rows + extra, :
                ]

    width = cols * len(parts)
    return whole_call(
        body,
        [
            jax.ShapeDtypeStruct((count * rows, width), parts[0].dtype),
            jax.ShapeDtypeStruct((count * extra, width), parts[0].dtype),
        ],
        me,
        *parts,
    )


def place_cols(pieces, me):
    count, (rows, cols) = len(pieces), pieces[0].shape

    def body(me_ref, *refs):
        for r in range(count):
            spot = pl.multiple_of((me_ref[0] ^ r) * cols, cols)
            refs[-1][:, pl.ds(spot, cols)] = refs[r][...]

    return whole_call(
        body, jax.ShapeDtypeStruct((rows, count * cols), pieces[0].dtype), me, *pieces
    )


def take_rows(value, extra, spans, orders, me):
    count = len(orders[0])
    rows = value.shape[0] // count
    more = 0 if extra is None else extra.shape[0] // count
    arrays = [value] if extra is None else [value, extra]

    def body(me_ref, *refs):
        sources, outs = refs[: len(arrays)], refs[len(arrays) :]
        for p, ((begin, end), order) in enumerate(zip(spans, orders)):
            for k, r in enumerate(order):
                out = outs[2 * p + (2 * k) // count]
                base = (k % (count // 2)) * (rows + more)
                here = me_ref[0] ^ r
                out[base : base + rows, :] = sources[0][
                    pl.ds(pl.multiple_of(here * rows, rows), rows), begin:end
                ]
                if more:
                    out[base + rows : base + rows + more, :] = sources[1][
                        pl.ds(pl.multiple_of(here * more, more), more), begin:end
                    ]

    outs = []
    for begin, end in spans:
        outs += [jax.ShapeDtypeStruct((count // 2 * (rows + more), end - begin), value.dtype)] * 2
    return whole_call(body, outs, me, *arrays)


def take_cols(value, order, groups, me):
    count = len(order)
    rows, cols = value.shape[0], value.shape[1] // count
    each = count // groups

    def body(me_ref, src, *outs):
        for k, r in enumerate(order):
            spot = pl.multiple_of((me_ref[0] ^ r) * cols, cols)
            base = (k % each) * rows
            outs[k // each][base : base + rows, :] = src[:, pl.ds(spot, cols)]

    return whole_call(
        body, [jax.ShapeDtypeStruct((each * rows, cols), value.dtype)] * groups, me, value
    )


def spread_cols(stacked, order, first, last, sections, me):
    count = len(order)
    rows = stacked.shape[0] // count
    cols = (last - first) // sections
    if cols % LANES:
        blocks = stacked.reshape(count, rows, -1)[:, :, first:last]
        blocks = blocks[jnp.argsort(jnp.array(order) ^ me)].reshape(count, rows, sections, cols)
        return blocks.transpose(1, 2, 0, 3).reshape(rows, -1).astype(F32)

    def body(me_ref, src, out):
        for k, r in enumerate(order):
            here = me_ref[0] ^ r
            for c in range(sections):
                spot = pl.multiple_of((c * count + here) * cols, cols)
                out[:, pl.ds(spot, cols)] = src[
                    k * rows : (k + 1) * rows, first + c * cols : first + (c + 1) * cols
                ].astype(F32)

    return whole_call(
        body, jax.ShapeDtypeStruct((rows, count * sections * cols), F32), me, stacked
    )


def spread_rows(stacked, order, first, last, me):
    count = len(order)
    rows = stacked.shape[0] // count

    def body(me_ref, src, out):
        for k, r in enumerate(order):
            spot = pl.multiple_of((me_ref[0] ^ r) * rows, rows)
            out[pl.ds(spot, rows), :] = src[k * rows : (k + 1) * rows, first:last].astype(F32)

    return whole_call(
        body, jax.ShapeDtypeStruct((count * rows, last - first), F32), me, stacked
    )


def pair_mask(shape, head):
    lane = lax.broadcasted_iota(jnp.int32, shape, 1)
    return (lane >= head * HEAD_DIM) & (lane < (head + 1) * HEAD_DIM)


def dot_nt(a, b):
    return lax.dot_general(a, b, (((1,), (1,)), ((), ())), preferred_element_type=F32)


def dot_nn(a, b):
    return lax.dot_general(a, b, (((1,), (0,)), ((), ())), preferred_element_type=F32)


def dot_tn(a, b):
    return lax.dot_general(a, b, (((0,), (0,)), ((), ())), preferred_element_type=F32)


def distance_tile(start_row, row_at, key_at, keys, rows):
    key = lax.broadcasted_iota(jnp.int32, (keys, rows), 0) + key_at
    row = lax.broadcasted_iota(jnp.int32, (keys, rows), 1) + row_at
    allowed = (key <= row) & (key >= start_row)
    return jnp.where(allowed, (key - row).astype(F32), MASKED)


def attend_body(block, low_ref, slope_ref, start_ref, q_ref, k_ref, v_ref, o_ref, lse_ref, m_ref, l_ref, acc_ref):
    pair, step = pl.program_id(0), pl.program_id(1)
    m_ref[...] = jnp.full_like(m_ref, -3e38)
    l_ref[...] = jnp.zeros_like(l_ref)
    acc_ref[...] = jnp.zeros_like(acc_ref)
    queries = q_ref[...]
    start_row = start_ref[...]
    heads = [jnp.where(pair_mask(queries.shape, h), queries, 0).astype(BF) for h in range(2)]

    def tile(j, _):
        at = pl.multiple_of(j * block, block)
        keys = k_ref[pl.ds(at, block), :]
        values = v_ref[pl.ds(at, block), :]
        dist = distance_tile(start_row, step * block, at, block, block)
        for h in range(2):
            scores = dot_nt(keys, heads[h]) + slope_ref[pair * 2 + h] * dist
            old = m_ref[h : h + 1, :]
            new = jnp.maximum(old, jnp.max(scores, axis=0, keepdims=True))
            shrink = jnp.exp(old - new)
            weight = jnp.exp(scores - new)
            m_ref[h : h + 1, :] = new
            l_ref[h : h + 1, :] = l_ref[h : h + 1, :] * shrink + jnp.sum(
                weight, axis=0, keepdims=True
            )
            acc_ref[h] = acc_ref[h] * shrink + dot_tn(values, weight.astype(BF))
        return 0

    lax.fori_loop(low_ref[step], step + 1, tile, 0)
    top = acc_ref[0] / l_ref[0:1, :]
    bottom = acc_ref[1] / l_ref[1:2, :]
    row = lax.broadcasted_iota(jnp.int32, top.shape, 0)
    o_ref[...] = jnp.where(row < HEAD_DIM, top, bottom).T.astype(BF)
    lse_ref[...] = (m_ref[...] + jnp.log(l_ref[...])).reshape(lse_ref.shape)


def attend(qkv, low, slopes, start, block):
    rows, width = qkv.shape[0], qkv.shape[1] // 3
    pairs = width // LANES
    return pl.pallas_call(
        functools.partial(attend_body, block),
        out_shape=(
            jax.ShapeDtypeStruct((rows, width), BF),
            jax.ShapeDtypeStruct((pairs, 2, rows), F32),
        ),
        grid=(pairs, rows // block),
        in_specs=[
            smem(),
            smem(),
            pl.BlockSpec((1, block), lambda p, i: (0, i)),
            pl.BlockSpec((block, LANES), lambda p, i: (i, p)),
            pl.BlockSpec((rows, LANES), lambda p, i: (0, pairs + p)),
            pl.BlockSpec((rows, LANES), lambda p, i: (0, 2 * pairs + p)),
        ],
        out_specs=(
            pl.BlockSpec((block, LANES), lambda p, i: (i, p)),
            pl.BlockSpec((1, 2, block), lambda p, i: (p, 0, i)),
        ),
        scratch_shapes=[
            pltpu.VMEM((2, block), F32),
            pltpu.VMEM((2, block), F32),
            pltpu.VMEM((2, LANES, block), F32),
        ],
        cost_estimate=pl.CostEstimate(
            flops=rows * rows * width, bytes_accessed=10 * rows * width, transcendentals=rows * rows
        ),
        name="attend",
    )(low, slopes, start, qkv, qkv, qkv)


def attend_back_body(
    block, low_ref, slope_ref, start_ref, lse_ref, q_ref, k_ref, v_ref, o_ref, g_ref, dq_ref, dk_ref, dv_ref, dq_acc, dk_acc, dv_acc
):
    pair, step = pl.program_id(0), pl.program_id(1)

    @pl.when(step == 0)
    def _():
        dk_acc[...] = jnp.zeros_like(dk_acc)
        dv_acc[...] = jnp.zeros_like(dv_acc)

    dq_acc[...] = jnp.zeros_like(dq_acc)
    queries, grads = q_ref[...], g_ref[...]
    start_row = start_ref[...]
    product = (o_ref[...].astype(F32) * grads.astype(F32)).T
    dots = [
        jnp.sum(product[h * HEAD_DIM : (h + 1) * HEAD_DIM], axis=0, keepdims=True) for h in range(2)
    ]
    masks = [pair_mask(queries.shape, h) for h in range(2)]
    q_heads = [jnp.where(m, queries, 0).astype(BF) for m in masks]
    g_heads = [jnp.where(m, grads, 0).astype(BF) for m in masks]

    def tile(j, _):
        at = pl.multiple_of(j * block, block)
        keys = k_ref[pl.ds(at, block), :]
        values = v_ref[pl.ds(at, block), :]
        dist = distance_tile(start_row, step * block, at, block, block)
        dk = dk_acc[pl.ds(at, block), :]
        dv = dv_acc[pl.ds(at, block), :]
        dq = dq_acc[...]
        for h in range(2):
            scores = dot_nt(keys, q_heads[h]) + slope_ref[pair * 2 + h] * dist
            prob = jnp.exp(scores - lse_ref[0, h : h + 1, :])
            dprob = dot_nt(values, g_heads[h])
            dscore = (prob * (dprob - dots[h])).astype(BF)
            dv += dot_nn(prob.astype(BF), g_heads[h])
            dk += dot_nn(dscore, q_heads[h])
            key_head = jnp.where(masks[h], keys, 0).astype(BF)
            dq += dot_tn(key_head, dscore)
        dk_acc[pl.ds(at, block), :] = dk
        dv_acc[pl.ds(at, block), :] = dv
        dq_acc[...] = dq
        return 0

    lax.fori_loop(low_ref[step], step + 1, tile, 0)
    dq_ref[...] = (dq_acc[...].T * (1.0 / math.sqrt(HEAD_DIM))).astype(BF)

    @pl.when(step == pl.num_programs(1) - 1)
    def _():
        dk_ref[...] = dk_acc[...].astype(BF)
        dv_ref[...] = dv_acc[...].astype(BF)


def attend_back(qkv, out, grad, lse, low, slopes, start, block):
    rows, width = qkv.shape[0], qkv.shape[1] // 3
    pairs = width // LANES
    return pl.pallas_call(
        functools.partial(attend_back_body, block),
        out_shape=[jax.ShapeDtypeStruct((rows, width), BF)] * 3,
        grid=(pairs, rows // block),
        in_specs=[
            smem(),
            smem(),
            pl.BlockSpec((1, block), lambda p, i: (0, i)),
            pl.BlockSpec((1, 2, block), lambda p, i: (p, 0, i)),
            pl.BlockSpec((block, LANES), lambda p, i: (i, p)),
            pl.BlockSpec((rows, LANES), lambda p, i: (0, pairs + p)),
            pl.BlockSpec((rows, LANES), lambda p, i: (0, 2 * pairs + p)),
            pl.BlockSpec((block, LANES), lambda p, i: (i, p)),
            pl.BlockSpec((block, LANES), lambda p, i: (i, p)),
        ],
        out_specs=[
            pl.BlockSpec((block, LANES), lambda p, i: (i, p)),
            pl.BlockSpec((rows, LANES), lambda p, i: (0, p)),
            pl.BlockSpec((rows, LANES), lambda p, i: (0, p)),
        ],
        scratch_shapes=[
            pltpu.VMEM((LANES, block), F32),
            pltpu.VMEM((rows, LANES), F32),
            pltpu.VMEM((rows, LANES), F32),
        ],
        cost_estimate=pl.CostEstimate(
            flops=3 * rows * rows * width, bytes_accessed=20 * rows * width, transcendentals=rows * rows
        ),
        name="attend_back",
    )(low, slopes, start, lse, qkv, qkv, qkv, out, grad)


def normalize(values):
    average = jnp.mean(values, axis=-1, keepdims=True)
    centered = values - average
    variance = jnp.mean(centered * centered, axis=-1, keepdims=True)
    scale = lax.rsqrt(variance + 1e-05)
    return centered * scale, scale


def norm_back(grad, gain, normed, scale):
    e = grad * gain
    return scale * (
        e
        - jnp.mean(e, axis=-1, keepdims=True)
        - normed * jnp.mean(e * normed, axis=-1, keepdims=True)
    )


def gelu_and_slope(v):
    c = math.sqrt(2 / math.pi)
    t = jnp.tanh(c * (v + 0.044715 * v * v * v))
    slope = 0.5 * (1 + t) + 0.5 * v * (1 - t * t) * c * (1 + 3 * 0.044715 * v * v)
    return 0.5 * v * (1 + t), slope


def mm(a, b):
    return jnp.dot(a, b, preferred_element_type=F32)


def mm_nt(a, b):
    return lax.dot_general(a, b, (((1,), (1,)), ((), ())), preferred_element_type=F32)


def mm_tn(a, b):
    return lax.dot_general(a, b, (((0,), (0,)), ((), ())), preferred_element_type=F32)


def shards(
    nf,
    ns,
    tokens,
    cotangent,
    seq_lengths,
    stream_order,
    first_gain,
    first_shift,
    qkv_weight,
    query_bias,
    value_bias,
    out_weight,
    out_bias,
    second_gain,
    second_shift,
    up_weight,
    up_bias,
    down_weight,
    down_bias,
):
    f, s = lax.axis_index("fsdp"), lax.axis_index("seq")
    toks, width = tokens.shape
    group = toks * ns
    dl, hl = width // nf, width // ns
    ff = up_weight.shape[1]
    ffl = ff // nf
    q = ffl // ns
    ffs = nf * q
    wide = 3 * hl
    bits_z = falling(nf)
    bits_y = bits_z[-1:] + bits_z[:-1]
    bits_s = falling(ns)
    f_orders = [order_of(bits_z), order_of(bits_y)]
    s_order = order_of(bits_s)
    back = lambda bits: tuple(reversed(bits))

    vectors = jnp.concatenate(
        [first_gain, first_shift, query_bias, value_bias, out_bias, second_gain, second_shift, down_bias, up_bias]
    )
    vec_rows = vectors.shape[0] // wide
    extra = 16
    qkv_shard = jnp.concatenate(
        [lax.dynamic_slice(qkv_weight, (0, k * width + s * hl), (dl, hl)) for k in range(3)], axis=1
    )
    qkv_shard = jnp.concatenate(
        [qkv_shard, vectors.reshape(vec_rows, wide), jnp.zeros((extra - vec_rows, wide), BF)], axis=0
    )
    qkv_parts = [
        gather_rows(qkv_shard[:, : wide // 2], "fsdp", nf, bits_z),
        gather_rows(qkv_shard[:, wide // 2 :], "fsdp", nf, bits_y),
    ]
    x_all = gather_rows(tokens, "seq", ns, bits_s)
    up_shard = lax.dynamic_index_in_dim(
        up_weight.reshape(dl, nf, ns, q), s, 2, keepdims=False
    ).reshape(dl, ffs)
    down_shard = lax.dynamic_slice(down_weight, (s * q, 0), (q, width))
    if q == dl:
        packed = jnp.concatenate([out_weight, up_shard, down_shard], axis=1)
        packed = lax.all_gather(packed, "fsdp", axis=0, tiled=True)
        out_full = packed[:, :width]
        up_full = packed[:, width : width + ffs]
        down_full = packed[:, width + ffs :]
    else:
        out_full = lax.all_gather(out_weight, "fsdp", axis=0, tiled=True)
        up_full = lax.all_gather(up_shard, "fsdp", axis=0, tiled=True)
        down_full = lax.all_gather(down_shard, "fsdp", axis=0, tiled=True)
    near = bits_s[-1:]
    far = bits_s[:-1]
    ct_near = gather_rows(cotangent, "seq", ns, near)
    ct_far = gather_rows(cotangent, "seq", ns, far)[toks:]
    ct_far = gather_rows(ct_far, "seq", ns, near)

    qkv_full, vec_all = place_weights(qkv_parts, f_orders, dl, extra, f)
    vecs = vec_all.reshape(nf, extra, wide)[:, :vec_rows].reshape(nf, -1, dl).astype(F32)
    full = vecs[:, :8].transpose(1, 0, 2).reshape(8, width)
    gain_one, shift_one, bias_query, bias_value, bias_out, gain_two, shift_two, bias_down = full
    bias_up = lax.dynamic_index_in_dim(vecs[:, 8:].reshape(nf, ns, q), s, 1, keepdims=False)
    bias_up = bias_up.reshape(ffs)
    bias_qkv = jnp.concatenate(
        [
            lax.dynamic_slice(bias_query, (s * hl,), (hl,)),
            jnp.zeros((hl,), F32),
            lax.dynamic_slice(bias_value, (s * hl,), (hl,)),
        ]
    )
    query_scale = jnp.where(jnp.arange(wide) < hl, 1.0 / math.sqrt(HEAD_DIM), 1.0)

    positions = stream_order[0].reshape(ns, toks)[jnp.array(s_order) ^ s].reshape(group)
    ends = jnp.cumsum(seq_lengths[0])
    line = jnp.arange(group)
    start = jnp.max(jnp.where(ends[None, :] <= line[:, None], ends[None, :], 0), axis=1)
    block = min(256, group)
    low = (start[::block] // block).astype(jnp.int32)
    start_row = start.astype(jnp.int32)[None, :]
    heads_here = hl // HEAD_DIM
    slopes = jnp.exp2(
        -(s * heads_here + 1 + jnp.arange(heads_here)).astype(F32) * (8.0 / HEADS)
    )
    to_sorted = (positions[None, :] == line[:, None]).astype(BF)

    n_all, _ = normalize(x_all.astype(F32))
    a_all = (n_all * gain_one + shift_one).astype(BF)
    qkv = ((mm(a_all, qkv_full) + bias_qkv).astype(BF).astype(F32) * query_scale).astype(BF)
    qkv_sorted = mm(to_sorted, qkv).astype(BF)
    o_sorted, lse = attend(qkv_sorted, low, slopes, start_row, block)
    context_heads = mm_tn(to_sorted, o_sorted).astype(BF)

    def exchange(blocks):
        return [blocks[0]] + [swap(blocks[r], "seq", ns, r) for r in range(1, ns)]

    context = place_cols(
        exchange([context_heads[k * toks : (k + 1) * toks] for k in (s_order.index(r) for r in range(ns))]), s
    )

    x_own = tokens.astype(F32)
    residual = x_own + mm(context, out_full) + bias_out
    n_two, scale_two = normalize(residual)
    m_low = (n_two * gain_two + shift_two).astype(BF)
    m_far = gather_rows(m_low, "seq", ns, far)[toks:]
    m_near = gather_rows(m_low, "seq", ns, near)
    m_far = gather_rows(m_far, "seq", ns, near)

    def feed_forward(m, ct):
        activated, slope = gelu_and_slope(mm(m, up_full) + bias_up)
        act = activated.astype(BF)
        d_pre = (mm_nt(ct, down_full) * slope).astype(BF)
        return act, d_pre, mm_nt(d_pre, up_full).astype(BF)

    act_near, d_pre_near, d_m_near = feed_forward(m_near, ct_near)
    act_far, d_pre_far, d_m_far = feed_forward(m_far, ct_far)

    def home(near_part, far_part):
        half = far_part.shape[0] // 2
        keep_near = near_part[:toks].astype(F32) + swap(near_part[toks:], "seq", ns, near[0]).astype(F32)
        keep_far = far_part[:half].astype(F32) + swap(far_part[half:], "seq", ns, near[0]).astype(F32)
        blocks = dict(zip(order_of(far)[1:], jnp.split(keep_far.astype(BF), ns // 2 - 1)))
        blocks[0] = keep_near
        for bit in back(far):
            for r in sorted(blocks):
                if r & bit:
                    arrived = swap(blocks.pop(r).astype(BF), "seq", ns, bit)
                    blocks[r ^ bit] = blocks[r ^ bit].astype(F32) + arrived.astype(F32)
        return blocks[0]

    d_m = home(d_m_near, d_m_far)
    total = home(mm(act_near, down_full).astype(BF), mm(act_far, down_full).astype(BF))
    output = (residual + total + bias_down).astype(BF)
    grad_up = (mm_tn(m_near, d_pre_near) + mm_tn(m_far, d_pre_far)).astype(BF)
    grad_down = (mm_tn(act_near, ct_near) + mm_tn(act_far, ct_far)).astype(BF)
    grad_up_bias = jnp.sum(d_pre_near, axis=0, dtype=F32) + jnp.sum(d_pre_far, axis=0, dtype=F32)

    def scatter_whole(value):
        return lax.psum_scatter(value, "fsdp", scatter_dimension=0, tiled=True)

    if q == dl:
        grad_ff = scatter_whole(jnp.concatenate([grad_up, grad_down], axis=1))
        grad_ff = gather_rows(grad_ff, "seq", ns, bits_s)
        up_all = spread_cols(grad_ff, s_order, 0, ffs, nf, s)
        down_all = spread_rows(grad_ff, s_order, ffs, ffs + width, s)
    else:
        grad_up = gather_rows(scatter_whole(grad_up), "seq", ns, bits_s)
        grad_down = gather_rows(scatter_whole(grad_down), "seq", ns, bits_s)
        up_all = spread_cols(grad_up, s_order, 0, ffs, nf, s)
        down_all = spread_rows(grad_down, s_order, 0, width, s)

    ct_own = cotangent.astype(F32)
    grad_down_bias = jnp.sum(ct_own, axis=0)
    grad_gain_two = jnp.sum(d_m * n_two, axis=0)
    grad_shift_two = jnp.sum(d_m, axis=0)
    d_res = ct_own + norm_back(d_m, gain_two, n_two, scale_two)
    d_att = d_res.astype(BF)
    grad_out_bias = jnp.sum(d_att, axis=0, dtype=F32)
    d_context = exchange(take_cols(mm_nt(d_att, out_full).astype(BF), list(range(ns)), ns, s))
    d_context = jnp.concatenate([d_context[r] for r in s_order], axis=0)
    d_o_sorted = mm(to_sorted, d_context).astype(BF)
    grad_out = take_cols(mm_tn(context, d_att).astype(BF), s_order, 2, s)
    grad_out = scatter_rows(*grad_out, "seq", ns, back(bits_s), BF)
    grad_out = take_rows(grad_out, None, [(0, hl)], f_orders[:1], f)
    grad_out = scatter_rows(*grad_out, "fsdp", nf, back(bits_z), BF)

    d_qkv_sorted = jnp.concatenate(
        attend_back(qkv_sorted, o_sorted, d_o_sorted, lse, low, slopes, start_row, block), axis=1
    )
    d_qkv = mm_tn(to_sorted, d_qkv_sorted).astype(BF)
    d_a_part = mm_nt(d_qkv, qkv_full)
    d_a_low = d_a_part.astype(BF)
    d_a = scatter_rows(d_a_low[: group // 2], d_a_low[group // 2 :], "seq", ns, back(bits_s))
    grad_qkv = mm_tn(a_all, d_qkv).astype(BF)
    grad_bias_qkv = jnp.sum(d_qkv, axis=0, dtype=F32)
    grad_gain_one = jnp.sum(d_a_part * n_all, axis=0)
    grad_shift_one = jnp.sum(d_a_part, axis=0)
    n_own, scale_own = normalize(x_own)
    tokens_grad = d_res + norm_back(d_a, gain_one, n_own, scale_own)

    def spread(part):
        return lax.dynamic_update_slice(jnp.zeros((width,), F32), part, (s * hl,))

    vec_part = jnp.stack(
        [
            grad_gain_one,
            grad_shift_one,
            spread(grad_bias_qkv[:hl]),
            spread(grad_bias_qkv[2 * hl :]),
            grad_out_bias,
            grad_gain_two,
            grad_shift_two,
            grad_down_bias,
        ]
    )
    vec_part = vec_part.reshape(8, nf, dl).transpose(1, 0, 2)
    up_part = lax.dynamic_update_slice(
        jnp.zeros((nf, ns, q), F32), grad_up_bias.reshape(nf, 1, q), (0, s, 0)
    ).reshape(nf, -1, dl)
    vec_part = jnp.concatenate([vec_part, up_part], axis=1).reshape(nf, vec_rows, wide)
    vec_part = jnp.pad(vec_part, ((0, 0), (0, extra - vec_rows), (0, 0))).astype(BF)
    vec_part = vec_part.reshape(nf * extra, wide)
    halves = [(0, wide // 2), (wide // 2, wide)]
    tail = take_rows(grad_qkv, vec_part, halves, f_orders, f)
    tail = [
        scatter_rows(tail[0], tail[1], "fsdp", nf, back(bits_z), BF),
        scatter_rows(tail[2], tail[3], "fsdp", nf, back(bits_y), BF),
        jnp.pad(grad_out, ((0, extra), (0, 0))),
    ]
    tail = gather_rows(jnp.concatenate(tail, axis=1), "seq", ns, bits_s)
    tail_rows = tail.reshape(ns, dl + extra, wide + hl)
    vec_sum = jnp.sum(tail_rows[:, dl : dl + vec_rows, :wide].astype(F32), axis=0).reshape(-1, dl)
    tail = tail_rows[:, :dl].reshape(ns * dl, wide + hl)
    qkv_all = spread_cols(tail, s_order, 0, wide, 3, s)
    out_all = spread_cols(tail, s_order, wide, wide + hl, 1, s)
    return (
        output,
        tokens_grad,
        vec_sum[0],
        vec_sum[1],
        qkv_all,
        vec_sum[2],
        vec_sum[3],
        out_all,
        vec_sum[4],
        vec_sum[5],
        vec_sum[6],
        up_all,
        vec_sum[8:].reshape(ffl),
        down_all,
        vec_sum[7],
    )


def solution(mesh):
    rows, cols, vec = P(("fsdp", "seq"), None), P("fsdp", None), P("fsdp")
    return jax.shard_map(
        functools.partial(shards, mesh.shape["fsdp"], mesh.shape["seq"]),
        mesh=mesh,
        in_specs=(rows, rows, cols, cols, vec, vec, cols, vec, vec, cols, vec, vec, vec, cols, vec, cols, vec),
        out_specs=(rows, rows, vec, vec, cols, vec, vec, cols, vec, vec, vec, cols, vec, cols, vec),
        check_vma=False,
    )
```

```python
import functools
import math

import jax
import jax.numpy as jnp
from jax import lax
from jax.experimental import pallas as pl
from jax.experimental.pallas import tpu as pltpu
from jax.sharding import PartitionSpec as P

HEADS = 16
HEAD_DIM = 64
LANES = 128
BF = jnp.bfloat16
F32 = jnp.float32
MASKED = -1e30


def swap(value, axis, size, bit):
    return lax.ppermute(value, axis, [(i, i ^ bit) for i in range(size)])


def falling(size):
    bits = []
    while size > 1:
        size //= 2
        bits.append(size)
    return tuple(bits)


def order_of(bits):
    order = [0]
    for bit in bits:
        order = order + [k ^ bit for k in order]
    return order


def gather_rows(value, axis, size, bits):
    for bit in bits:
        value = jnp.concatenate([value, swap(value, axis, size, bit)], axis=0)
    return value


def scatter_rows(keep, send, axis, size, bits, last=F32):
    for k, bit in enumerate(bits):
        arrived = swap(send, axis, size, bit)
        if k == len(bits) - 1:
            return (keep.astype(F32) + arrived.astype(F32)).astype(last)
        half = keep.shape[0] // 2
        send = (keep[half:].astype(F32) + arrived[half:].astype(F32)).astype(keep.dtype)
        keep = (keep[:half].astype(F32) + arrived[:half].astype(F32)).astype(keep.dtype)


def vmem():
    return pl.BlockSpec(memory_space=pltpu.VMEM)


def smem():
    return pl.BlockSpec(memory_space=pltpu.SMEM)


def whole_call(body, outs, me, *arrays):
    return pl.pallas_call(
        body,
        out_shape=outs,
        in_specs=[smem()] + [vmem()] * len(arrays),
        out_specs=jax.tree.map(lambda _: vmem(), outs),
    )(me.reshape(1).astype(jnp.int32), *arrays)


def remote(src, dst, sems, at, axis, target):
    return pltpu.make_async_remote_copy(
        src_ref=src,
        dst_ref=dst,
        send_sem=sems[0].at[at],
        recv_sem=sems[1].at[at],
        device_id={axis: target},
        device_id_type=pl.DeviceIdType.MESH,
    )


def low_part(size):
    return 2 if size <= 8 else 4


def greet(peers):
    barrier = pltpu.get_barrier_semaphore()
    for axis, target in peers:
        pl.semaphore_signal(
            barrier, inc=1, device_id={axis: target}, device_id_type=pl.DeviceIdType.MESH
        )
    pl.semaphore_wait(barrier, len(peers))


def peers_of(axis, size, lo):
    me = lax.axis_index(axis)
    far = [(axis, me ^ (d * lo)) for d in range(1, size // lo)]
    return far + [(axis, me ^ e) for e in range(1, lo)]


def farthest_first(count):
    return sorted(range(1, count), key=lambda d: -d)


def at_block(ref, index, rows):
    if isinstance(index, int):
        return ref.at[pl.ds(index * rows, rows)]
    return ref.at[pl.ds(pl.multiple_of(index * rows, rows), rows)]


class Gather:
    def __init__(self, src, dst, slot, axis, size, lo, far_sems, near_sems):
        me = lax.axis_index(axis)
        hi, rows = size // lo, src.shape[0]
        self.src, self.dst, self.rows, self.own = src, dst, rows, slot(0, 0, me)
        self.far, self.near = {}, {}
        for d in range(1, hi):
            target = me ^ (d * lo)
            self.far[d] = remote(src, at_block(dst, slot(d, 0, target), rows), far_sems, d - 1, axis, target)
        for d in range(hi):
            origin = src if d == 0 else at_block(dst, slot(d, 0, me), rows)
            for e in range(1, lo):
                target = me ^ e
                self.near[d, e] = remote(
                    origin, at_block(dst, slot(d, e, target), rows), near_sems, d * (lo - 1) + e - 1, axis, target
                )

    def start(self):
        for d in farthest_first(len(self.far) + 1):
            self.far[d].start()
        self.pass_on(0)

    def arrive(self, d):
        self.far[d].wait_recv()
        self.pass_on(d)

    def pass_on(self, d):
        for (at, _), copy in self.near.items():
            if at == d:
                copy.start()

    def arrivals(self):
        return sorted(self.far)

    def finish(self):
        for copy in self.near.values():
            copy.wait_recv()
            copy.wait_send()
        for copy in self.far.values():
            copy.wait_send()


def gather_sems(size, lo, arrays):
    hi = size // lo
    kinds = []
    for _ in range(arrays):
        kinds += [pltpu.SemaphoreType.DMA((max(hi - 1, 1),))] * 2
        kinds += [pltpu.SemaphoreType.DMA((hi * (lo - 1),))] * 2
    return kinds


def head_body(nf, ns, s_order, w, v, x, w_all, v_all, x_all, *sems):
    lf, ls = low_part(nf), 2
    greet(peers_of("fsdp", nf, lf) + peers_of("seq", ns, ls))
    absolute = lambda d, e, me: me ^ (d * lf + e)
    relative = lambda d, e, me: s_order.index(d * ls + e)
    moves = []
    for k, (src, dst) in enumerate([(w, w_all), (v, v_all)]):
        moves.append(Gather(src, dst, absolute, "fsdp", nf, lf, sems[4 * k : 4 * k + 2], sems[4 * k + 2 : 4 * k + 4]))
    moves.append(Gather(x, x_all, relative, "seq", ns, ls, sems[8:10], sems[10:12]))
    for move in moves:
        move.start()
    me = lax.axis_index("fsdp")
    w_all[pl.ds(pl.multiple_of(me * w.shape[0], w.shape[0]), w.shape[0]), :] = w[...]
    v_all[pl.ds(pl.multiple_of(me * v.shape[0], v.shape[0]), v.shape[0]), :] = v[...]
    x_all[0 : x.shape[0], :] = x[...]
    for d in moves[0].arrivals():
        moves[0].arrive(d)
        moves[1].arrive(d)
    for d in moves[2].arrivals():
        moves[2].arrive(d)
    for move in moves:
        move.finish()


def head(nf, ns, s_order, w, v, x):
    return pl.pallas_call(
        functools.partial(head_body, nf, ns, s_order),
        out_shape=[
            jax.ShapeDtypeStruct((a.shape[0] * n, a.shape[1]), a.dtype) for a, n in ((w, nf), (v, nf), (x, ns))
        ],
        in_specs=[vmem()] * 3,
        out_specs=[vmem()] * 3,
        scratch_shapes=gather_sems(nf, low_part(nf), 2) + gather_sems(ns, 2, 1),
        compiler_params=pltpu.CompilerParams(collective_id=1, has_side_effects=True),
        name="head",
    )(w, v, x)


def tail_body(nf, ns, extra, g, v, o, qkv_out, vec_out, out_out, *rest):
    lf, ls = low_part(nf), 2
    hi = nf // lf
    arrays = [g, v, o]
    rest = list(rest)
    take = lambda count: [rest.pop(0) for _ in range(count)]
    near_in, summed, far_in, mine, everyone = take(3), take(3), take(3), take(3), take(3)
    near_sems, far_sems = [take(2) for _ in arrays], [take(2) for _ in arrays]
    seq_sems = [take(4) for _ in arrays]
    me = lax.axis_index("fsdp")
    greet(peers_of("fsdp", nf, lf) + peers_of("seq", ns, ls))
    order = farthest_first(hi) + [0]
    rows = [a.shape[0] // nf for a in arrays]
    near, far = {}, {}
    for d in order:
        for e in range(1, lf):
            for k, a in enumerate(arrays):
                at = d * (lf - 1) + e - 1
                near[d, e, k] = remote(
                    at_block(a, me ^ (d * lf + e), rows[k]), near_in[k].at[at], near_sems[k], at, "fsdp", me ^ e
                )
                near[d, e, k].start()
    for d in order:
        for k, a in enumerate(arrays):
            spot = pl.ds(pl.multiple_of((me ^ (d * lf)) * rows[k], rows[k]), rows[k])
            total = a[spot, :].astype(F32)
            for e in range(1, lf):
                near[d, e, k].wait_recv()
                total += near_in[k][d * (lf - 1) + e - 1].astype(F32)
            summed[k][d] = total.astype(BF)
            if d:
                far[d, k] = remote(
                    summed[k].at[d], far_in[k].at[d - 1], far_sems[k], d - 1, "fsdp", me ^ (d * lf)
                )
                far[d, k].start()
    moves = []
    for k, a in enumerate(arrays):
        total = summed[k][0].astype(F32)
        for d in range(1, hi):
            far[d, k].wait_recv()
            total += far_in[k][d - 1].astype(F32)
        mine[k][...] = total.astype(BF)
        relative = lambda d, e, _: d * ls + e
        moves.append(
            Gather(mine[k], everyone[k], relative, "seq", ns, ls, seq_sems[k][:2], seq_sems[k][2:])
        )
        moves[k].start()
    for d in moves[0].arrivals():
        for move in moves:
            move.arrive(d)
    for move in moves:
        move.finish()
    for copy in list(near.values()) + list(far.values()):
        copy.wait_send()
    seq = lax.axis_index("seq")
    hl = o.shape[1]
    vec_total = mine[1][...].astype(F32)
    for r in range(ns):
        here = seq ^ r
        sources = [mine[k] if r == 0 else at_block(everyone[k], r, rows[k]) for k in range(3)]
        for c in range(3):
            spot = pl.multiple_of((c * ns + here) * hl, hl)
            qkv_out[:, pl.ds(spot, hl)] = sources[0][:, c * hl : (c + 1) * hl].astype(F32)
        out_out[:, pl.ds(pl.multiple_of(here * hl, hl), hl)] = sources[2][...].astype(F32)
        if r:
            vec_total += sources[1][...].astype(F32)
    vec_out[...] = vec_total


def tail_call(nf, ns, g, v, o):
    lf = low_part(nf)
    hi = nf // lf
    arrays = [g, v, o]
    blocks = [(a.shape[0] // nf, a.shape[1]) for a in arrays]
    extra = blocks[1][0]
    scratch = []
    for lead in (hi * (lf - 1), hi, max(hi - 1, 1)):
        scratch += [pltpu.VMEM((lead,) + b, BF) for b in blocks]
    scratch += [pltpu.VMEM(b, BF) for b in blocks]
    scratch += [pltpu.VMEM((ns * b[0], b[1]), BF) for b in blocks]
    scratch += [pltpu.SemaphoreType.DMA((hi * (lf - 1),))] * 6
    scratch += [pltpu.SemaphoreType.DMA((max(hi - 1, 1),))] * 6
    scratch += gather_sems(ns, 2, 3)
    return pl.pallas_call(
        functools.partial(tail_body, nf, ns, extra),
        out_shape=[
            jax.ShapeDtypeStruct((blocks[0][0], ns * g.shape[1]), F32),
            jax.ShapeDtypeStruct(blocks[1], F32),
            jax.ShapeDtypeStruct((blocks[2][0], ns * o.shape[1]), F32),
        ],
        in_specs=[vmem()] * 3,
        out_specs=[vmem()] * 3,
        scratch_shapes=scratch,
        compiler_params=pltpu.CompilerParams(collective_id=2, has_side_effects=True),
        name="tail",
    )(g, v, o)


def place_cols(pieces, me):
    count, (rows, cols) = len(pieces), pieces[0].shape

    def body(me_ref, *refs):
        for r in range(count):
            spot = pl.multiple_of((me_ref[0] ^ r) * cols, cols)
            refs[-1][:, pl.ds(spot, cols)] = refs[r][...]

    return whole_call(
        body, jax.ShapeDtypeStruct((rows, count * cols), pieces[0].dtype), me, *pieces
    )


def take_cols(value, order, groups, me):
    count = len(order)
    rows, cols = value.shape[0], value.shape[1] // count
    each = count // groups

    def body(me_ref, src, *outs):
        for k, r in enumerate(order):
            spot = pl.multiple_of((me_ref[0] ^ r) * cols, cols)
            base = (k % each) * rows
            outs[k // each][base : base + rows, :] = src[:, pl.ds(spot, cols)]

    return whole_call(
        body, [jax.ShapeDtypeStruct((each * rows, cols), value.dtype)] * groups, me, value
    )


def spread_cols(stacked, order, first, last, sections, me):
    count = len(order)
    rows = stacked.shape[0] // count
    cols = (last - first) // sections
    if cols % LANES:
        blocks = stacked.reshape(count, rows, -1)[:, :, first:last]
        blocks = blocks[jnp.argsort(jnp.array(order) ^ me)].reshape(count, rows, sections, cols)
        return blocks.transpose(1, 2, 0, 3).reshape(rows, -1).astype(F32)

    def body(me_ref, src, out):
        for k, r in enumerate(order):
            here = me_ref[0] ^ r
            for c in range(sections):
                spot = pl.multiple_of((c * count + here) * cols, cols)
                out[:, pl.ds(spot, cols)] = src[
                    k * rows : (k + 1) * rows, first + c * cols : first + (c + 1) * cols
                ].astype(F32)

    return whole_call(
        body, jax.ShapeDtypeStruct((rows, count * sections * cols), F32), me, stacked
    )


def spread_rows(stacked, order, first, last, me):
    count = len(order)
    rows = stacked.shape[0] // count

    def body(me_ref, src, out):
        for k, r in enumerate(order):
            spot = pl.multiple_of((me_ref[0] ^ r) * rows, rows)
            out[pl.ds(spot, rows), :] = src[k * rows : (k + 1) * rows, first:last].astype(F32)

    return whole_call(
        body, jax.ShapeDtypeStruct((count * rows, last - first), F32), me, stacked
    )


def pair_mask(shape, head):
    lane = lax.broadcasted_iota(jnp.int32, shape, 1)
    return (lane >= head * HEAD_DIM) & (lane < (head + 1) * HEAD_DIM)


def dot_nt(a, b):
    return lax.dot_general(a, b, (((1,), (1,)), ((), ())), preferred_element_type=F32)


def dot_nn(a, b):
    return lax.dot_general(a, b, (((1,), (0,)), ((), ())), preferred_element_type=F32)


def dot_tn(a, b):
    return lax.dot_general(a, b, (((0,), (0,)), ((), ())), preferred_element_type=F32)


def distance_tile(start_row, row_at, key_at, keys, rows):
    key = lax.broadcasted_iota(jnp.int32, (keys, rows), 0) + key_at
    row = lax.broadcasted_iota(jnp.int32, (keys, rows), 1) + row_at
    allowed = (key <= row) & (key >= start_row)
    return jnp.where(allowed, (key - row).astype(F32), MASKED)


def attend_body(block, low_ref, slope_ref, start_ref, q_ref, k_ref, v_ref, o_ref, lse_ref, m_ref, l_ref, acc_ref):
    pair, step = pl.program_id(0), pl.program_id(1)
    m_ref[...] = jnp.full_like(m_ref, -3e38)
    l_ref[...] = jnp.zeros_like(l_ref)
    acc_ref[...] = jnp.zeros_like(acc_ref)
    queries = q_ref[...]
    start_row = start_ref[...]
    heads = [jnp.where(pair_mask(queries.shape, h), queries, 0).astype(BF) for h in range(2)]

    def tile(j, _):
        at = pl.multiple_of(j * block, block)
        keys = k_ref[pl.ds(at, block), :]
        values = v_ref[pl.ds(at, block), :]
        dist = distance_tile(start_row, step * block, at, block, block)
        for h in range(2):
            scores = dot_nt(keys, heads[h]) + slope_ref[pair * 2 + h] * dist
            old = m_ref[h : h + 1, :]
            new = jnp.maximum(old, jnp.max(scores, axis=0, keepdims=True))
            shrink = jnp.exp(old - new)
            weight = jnp.exp(scores - new)
            m_ref[h : h + 1, :] = new
            l_ref[h : h + 1, :] = l_ref[h : h + 1, :] * shrink + jnp.sum(
                weight, axis=0, keepdims=True
            )
            acc_ref[h] = acc_ref[h] * shrink + dot_tn(values, weight.astype(BF))
        return 0

    lax.fori_loop(low_ref[step], step + 1, tile, 0)
    top = acc_ref[0] / l_ref[0:1, :]
    bottom = acc_ref[1] / l_ref[1:2, :]
    row = lax.broadcasted_iota(jnp.int32, top.shape, 0)
    o_ref[...] = jnp.where(row < HEAD_DIM, top, bottom).T.astype(BF)
    lse_ref[...] = (m_ref[...] + jnp.log(l_ref[...])).reshape(lse_ref.shape)


def attend(qkv, low, slopes, start, block):
    rows, width = qkv.shape[0], qkv.shape[1] // 3
    pairs = width // LANES
    return pl.pallas_call(
        functools.partial(attend_body, block),
        out_shape=(
            jax.ShapeDtypeStruct((rows, width), BF),
            jax.ShapeDtypeStruct((pairs, 2, rows), F32),
        ),
        grid=(pairs, rows // block),
        in_specs=[
            smem(),
            smem(),
            pl.BlockSpec((1, block), lambda p, i: (0, i)),
            pl.BlockSpec((block, LANES), lambda p, i: (i, p)),
            pl.BlockSpec((rows, LANES), lambda p, i: (0, pairs + p)),
            pl.BlockSpec((rows, LANES), lambda p, i: (0, 2 * pairs + p)),
        ],
        out_specs=(
            pl.BlockSpec((block, LANES), lambda p, i: (i, p)),
            pl.BlockSpec((1, 2, block), lambda p, i: (p, 0, i)),
        ),
        scratch_shapes=[
            pltpu.VMEM((2, block), F32),
            pltpu.VMEM((2, block), F32),
            pltpu.VMEM((2, LANES, block), F32),
        ],
        cost_estimate=pl.CostEstimate(
            flops=rows * rows * width, bytes_accessed=10 * rows * width, transcendentals=rows * rows
        ),
        name="attend",
    )(low, slopes, start, qkv, qkv, qkv)


def attend_back_body(
    block, low_ref, slope_ref, start_ref, lse_ref, q_ref, k_ref, v_ref, o_ref, g_ref, dq_ref, dk_ref, dv_ref, dq_acc, dk_acc, dv_acc
):
    pair, step = pl.program_id(0), pl.program_id(1)

    @pl.when(step == 0)
    def _():
        dk_acc[...] = jnp.zeros_like(dk_acc)
        dv_acc[...] = jnp.zeros_like(dv_acc)

    dq_acc[...] = jnp.zeros_like(dq_acc)
    queries, grads = q_ref[...], g_ref[...]
    start_row = start_ref[...]
    product = (o_ref[...].astype(F32) * grads.astype(F32)).T
    dots = [
        jnp.sum(product[h * HEAD_DIM : (h + 1) * HEAD_DIM], axis=0, keepdims=True) for h in range(2)
    ]
    masks = [pair_mask(queries.shape, h) for h in range(2)]
    q_heads = [jnp.where(m, queries, 0).astype(BF) for m in masks]
    g_heads = [jnp.where(m, grads, 0).astype(BF) for m in masks]

    def tile(j, _):
        at = pl.multiple_of(j * block, block)
        keys = k_ref[pl.ds(at, block), :]
        values = v_ref[pl.ds(at, block), :]
        dist = distance_tile(start_row, step * block, at, block, block)
        dk = dk_acc[pl.ds(at, block), :]
        dv = dv_acc[pl.ds(at, block), :]
        dq = dq_acc[...]
        for h in range(2):
            scores = dot_nt(keys, q_heads[h]) + slope_ref[pair * 2 + h] * dist
            prob = jnp.exp(scores - lse_ref[0, h : h + 1, :])
            dprob = dot_nt(values, g_heads[h])
            dscore = (prob * (dprob - dots[h])).astype(BF)
            dv += dot_nn(prob.astype(BF), g_heads[h])
            dk += dot_nn(dscore, q_heads[h])
            key_head = jnp.where(masks[h], keys, 0).astype(BF)
            dq += dot_tn(key_head, dscore)
        dk_acc[pl.ds(at, block), :] = dk
        dv_acc[pl.ds(at, block), :] = dv
        dq_acc[...] = dq
        return 0

    lax.fori_loop(low_ref[step], step + 1, tile, 0)
    dq_ref[...] = (dq_acc[...].T * (1.0 / math.sqrt(HEAD_DIM))).astype(BF)

    @pl.when(step == pl.num_programs(1) - 1)
    def _():
        dk_ref[...] = dk_acc[...].astype(BF)
        dv_ref[...] = dv_acc[...].astype(BF)


def attend_back(qkv, out, grad, lse, low, slopes, start, block):
    rows, width = qkv.shape[0], qkv.shape[1] // 3
    pairs = width // LANES
    return pl.pallas_call(
        functools.partial(attend_back_body, block),
        out_shape=[jax.ShapeDtypeStruct((rows, width), BF)] * 3,
        grid=(pairs, rows // block),
        in_specs=[
            smem(),
            smem(),
            pl.BlockSpec((1, block), lambda p, i: (0, i)),
            pl.BlockSpec((1, 2, block), lambda p, i: (p, 0, i)),
            pl.BlockSpec((block, LANES), lambda p, i: (i, p)),
            pl.BlockSpec((rows, LANES), lambda p, i: (0, pairs + p)),
            pl.BlockSpec((rows, LANES), lambda p, i: (0, 2 * pairs + p)),
            pl.BlockSpec((block, LANES), lambda p, i: (i, p)),
            pl.BlockSpec((block, LANES), lambda p, i: (i, p)),
        ],
        out_specs=[
            pl.BlockSpec((block, LANES), lambda p, i: (i, p)),
            pl.BlockSpec((rows, LANES), lambda p, i: (0, p)),
            pl.BlockSpec((rows, LANES), lambda p, i: (0, p)),
        ],
        scratch_shapes=[
            pltpu.VMEM((LANES, block), F32),
            pltpu.VMEM((rows, LANES), F32),
            pltpu.VMEM((rows, LANES), F32),
        ],
        cost_estimate=pl.CostEstimate(
            flops=3 * rows * rows * width, bytes_accessed=20 * rows * width, transcendentals=rows * rows
        ),
        name="attend_back",
    )(low, slopes, start, lse, qkv, qkv, qkv, out, grad)


def normalize(values):
    average = jnp.mean(values, axis=-1, keepdims=True)
    centered = values - average
    variance = jnp.mean(centered * centered, axis=-1, keepdims=True)
    scale = lax.rsqrt(variance + 1e-05)
    return centered * scale, scale


def norm_back(grad, gain, normed, scale):
    e = grad * gain
    return scale * (
        e
        - jnp.mean(e, axis=-1, keepdims=True)
        - normed * jnp.mean(e * normed, axis=-1, keepdims=True)
    )


def gelu_and_slope(v):
    c = math.sqrt(2 / math.pi)
    t = jnp.tanh(c * (v + 0.044715 * v * v * v))
    slope = 0.5 * (1 + t) + 0.5 * v * (1 - t * t) * c * (1 + 3 * 0.044715 * v * v)
    return 0.5 * v * (1 + t), slope


def mm(a, b):
    return jnp.dot(a, b, preferred_element_type=F32)


def mm_nt(a, b):
    return lax.dot_general(a, b, (((1,), (1,)), ((), ())), preferred_element_type=F32)


def mm_tn(a, b):
    return lax.dot_general(a, b, (((0,), (0,)), ((), ())), preferred_element_type=F32)


def shards(
    nf,
    ns,
    tokens,
    cotangent,
    seq_lengths,
    stream_order,
    first_gain,
    first_shift,
    qkv_weight,
    query_bias,
    value_bias,
    out_weight,
    out_bias,
    second_gain,
    second_shift,
    up_weight,
    up_bias,
    down_weight,
    down_bias,
):
    f, s = lax.axis_index("fsdp"), lax.axis_index("seq")
    toks, width = tokens.shape
    group = toks * ns
    dl, hl = width // nf, width // ns
    ff = up_weight.shape[1]
    ffl = ff // nf
    q = ffl // ns
    ffs = nf * q
    wide = 3 * hl
    bits_s = falling(ns)
    s_order = order_of(bits_s)
    back = lambda bits: tuple(reversed(bits))

    vectors = jnp.concatenate(
        [first_gain, first_shift, query_bias, value_bias, out_bias, second_gain, second_shift, down_bias, up_bias]
    )
    vec_rows = vectors.shape[0] // wide
    extra = 16
    qkv_shard = jnp.concatenate(
        [lax.dynamic_slice(qkv_weight, (0, k * width + s * hl), (dl, hl)) for k in range(3)], axis=1
    )
    vec_shard = jnp.pad(vectors.reshape(vec_rows, wide), ((0, extra - vec_rows), (0, 0)))
    qkv_full, vec_all, x_all = head(nf, ns, s_order, qkv_shard, vec_shard, tokens)
    up_shard = lax.dynamic_index_in_dim(
        up_weight.reshape(dl, nf, ns, q), s, 2, keepdims=False
    ).reshape(dl, ffs)
    down_shard = lax.dynamic_slice(down_weight, (s * q, 0), (q, width))
    if q == dl:
        packed = jnp.concatenate([out_weight, up_shard, down_shard], axis=1)
        packed = lax.all_gather(packed, "fsdp", axis=0, tiled=True)
        out_full = packed[:, :width]
        up_full = packed[:, width : width + ffs]
        down_full = packed[:, width + ffs :]
    else:
        out_full = lax.all_gather(out_weight, "fsdp", axis=0, tiled=True)
        up_full = lax.all_gather(up_shard, "fsdp", axis=0, tiled=True)
        down_full = lax.all_gather(down_shard, "fsdp", axis=0, tiled=True)
    near = bits_s[-1:]
    far = bits_s[:-1]
    ct_near = gather_rows(cotangent, "seq", ns, near)
    ct_far = gather_rows(cotangent, "seq", ns, far)[toks:]
    ct_far = gather_rows(ct_far, "seq", ns, near)

    vecs = vec_all.reshape(nf, extra, wide)[:, :vec_rows].reshape(nf, -1, dl).astype(F32)
    full = vecs[:, :8].transpose(1, 0, 2).reshape(8, width)
    gain_one, shift_one, bias_query, bias_value, bias_out, gain_two, shift_two, bias_down = full
    bias_up = lax.dynamic_index_in_dim(vecs[:, 8:].reshape(nf, ns, q), s, 1, keepdims=False)
    bias_up = bias_up.reshape(ffs)
    bias_qkv = jnp.concatenate(
        [
            lax.dynamic_slice(bias_query, (s * hl,), (hl,)),
            jnp.zeros((hl,), F32),
            lax.dynamic_slice(bias_value, (s * hl,), (hl,)),
        ]
    )
    query_scale = jnp.where(jnp.arange(wide) < hl, 1.0 / math.sqrt(HEAD_DIM), 1.0)

    positions = stream_order[0].reshape(ns, toks)[jnp.array(s_order) ^ s].reshape(group)
    ends = jnp.cumsum(seq_lengths[0])
    line = jnp.arange(group)
    start = jnp.max(jnp.where(ends[None, :] <= line[:, None], ends[None, :], 0), axis=1)
    block = min(256, group)
    low = (start[::block] // block).astype(jnp.int32)
    start_row = start.astype(jnp.int32)[None, :]
    heads_here = hl // HEAD_DIM
    slopes = jnp.exp2(
        -(s * heads_here + 1 + jnp.arange(heads_here)).astype(F32) * (8.0 / HEADS)
    )
    to_sorted = (positions[None, :] == line[:, None]).astype(BF)

    n_all, _ = normalize(x_all.astype(F32))
    a_all = (n_all * gain_one + shift_one).astype(BF)
    qkv = ((mm(a_all, qkv_full) + bias_qkv).astype(BF).astype(F32) * query_scale).astype(BF)
    qkv_sorted = mm(to_sorted, qkv).astype(BF)
    o_sorted, lse = attend(qkv_sorted, low, slopes, start_row, block)
    context_heads = mm_tn(to_sorted, o_sorted).astype(BF)

    def exchange(blocks):
        return [blocks[0]] + [swap(blocks[r], "seq", ns, r) for r in range(1, ns)]

    context = place_cols(
        exchange([context_heads[k * toks : (k + 1) * toks] for k in (s_order.index(r) for r in range(ns))]), s
    )

    x_own = tokens.astype(F32)
    residual = x_own + mm(context, out_full) + bias_out
    n_two, scale_two = normalize(residual)
    m_low = (n_two * gain_two + shift_two).astype(BF)
    m_far = gather_rows(m_low, "seq", ns, far)[toks:]
    m_near = gather_rows(m_low, "seq", ns, near)
    m_far = gather_rows(m_far, "seq", ns, near)

    def feed_forward(m, ct):
        activated, slope = gelu_and_slope(mm(m, up_full) + bias_up)
        act = activated.astype(BF)
        d_pre = (mm_nt(ct, down_full) * slope).astype(BF)
        return act, d_pre, mm_nt(d_pre, up_full).astype(BF)

    act_near, d_pre_near, d_m_near = feed_forward(m_near, ct_near)
    act_far, d_pre_far, d_m_far = feed_forward(m_far, ct_far)

    def home_near(near_part, far_part):
        half = far_part.shape[0] // 2
        keep_near = near_part[:toks].astype(F32) + swap(near_part[toks:], "seq", ns, near[0]).astype(F32)
        keep_far = far_part[:half].astype(F32) + swap(far_part[half:], "seq", ns, near[0]).astype(F32)
        return keep_near, keep_far.astype(BF)

    def home_far(keep_near, keep_far):
        blocks = dict(zip(order_of(far)[1:], jnp.split(keep_far, ns // 2 - 1)))
        blocks[0] = keep_near
        for bit in back(far):
            for r in sorted(blocks):
                if r & bit:
                    arrived = swap(blocks.pop(r).astype(BF), "seq", ns, bit)
                    blocks[r ^ bit] = blocks[r ^ bit].astype(F32) + arrived.astype(F32)
        return blocks[0]

    d_m = home_far(*home_near(d_m_near, d_m_far))
    total_near, total_far = home_near(mm(act_near, down_full).astype(BF), mm(act_far, down_full).astype(BF))
    grad_up = (mm_tn(m_near, d_pre_near) + mm_tn(m_far, d_pre_far)).astype(BF)
    grad_down = (mm_tn(act_near, ct_near) + mm_tn(act_far, ct_far)).astype(BF)
    grad_up_bias = jnp.sum(d_pre_near, axis=0, dtype=F32) + jnp.sum(d_pre_far, axis=0, dtype=F32)

    def scatter_whole(value):
        return lax.psum_scatter(value, "fsdp", scatter_dimension=0, tiled=True)

    if q == dl:
        grad_ff = scatter_whole(jnp.concatenate([grad_up, grad_down], axis=1))
        grad_ff = gather_rows(grad_ff, "seq", ns, bits_s)
        up_all = spread_cols(grad_ff, s_order, 0, ffs, nf, s)
        down_all = spread_rows(grad_ff, s_order, ffs, ffs + width, s)
    else:
        grad_up = gather_rows(scatter_whole(grad_up), "seq", ns, bits_s)
        grad_down = gather_rows(scatter_whole(grad_down), "seq", ns, bits_s)
        up_all = spread_cols(grad_up, s_order, 0, ffs, nf, s)
        down_all = spread_rows(grad_down, s_order, 0, width, s)

    ct_own = cotangent.astype(F32)
    grad_down_bias = jnp.sum(ct_own, axis=0)
    grad_gain_two = jnp.sum(d_m * n_two, axis=0)
    grad_shift_two = jnp.sum(d_m, axis=0)
    d_res = ct_own + norm_back(d_m, gain_two, n_two, scale_two)
    d_att = d_res.astype(BF)
    grad_out_bias = jnp.sum(d_att, axis=0, dtype=F32)
    d_context = exchange(take_cols(mm_nt(d_att, out_full).astype(BF), list(range(ns)), ns, s))
    d_context = jnp.concatenate([d_context[r] for r in s_order], axis=0)
    total_near, total_far, d_context = lax.optimization_barrier((total_near, total_far, d_context))
    output = (residual + home_far(total_near, total_far) + bias_down).astype(BF)
    d_o_sorted = mm(to_sorted, d_context).astype(BF)
    grad_out = take_cols(mm_tn(context, d_att).astype(BF), s_order, 2, s)
    grad_out = scatter_rows(*grad_out, "seq", ns, back(bits_s), BF)

    d_qkv_sorted = jnp.concatenate(
        attend_back(qkv_sorted, o_sorted, d_o_sorted, lse, low, slopes, start_row, block), axis=1
    )
    d_qkv = mm_tn(to_sorted, d_qkv_sorted).astype(BF)
    d_a_part = mm_nt(d_qkv, qkv_full)
    d_a_low = d_a_part.astype(BF)
    d_a = scatter_rows(d_a_low[: group // 2], d_a_low[group // 2 :], "seq", ns, back(bits_s))
    grad_qkv = mm_tn(a_all, d_qkv).astype(BF)
    grad_bias_qkv = jnp.sum(d_qkv, axis=0, dtype=F32)
    grad_gain_one = jnp.sum(d_a_part * n_all, axis=0)
    grad_shift_one = jnp.sum(d_a_part, axis=0)
    n_own, scale_own = normalize(x_own)
    tokens_grad = d_res + norm_back(d_a, gain_one, n_own, scale_own)

    def spread(part):
        return lax.dynamic_update_slice(jnp.zeros((width,), F32), part, (s * hl,))

    vec_part = jnp.stack(
        [
            grad_gain_one,
            grad_shift_one,
            spread(grad_bias_qkv[:hl]),
            spread(grad_bias_qkv[2 * hl :]),
            grad_out_bias,
            grad_gain_two,
            grad_shift_two,
            grad_down_bias,
        ]
    )
    vec_part = vec_part.reshape(8, nf, dl).transpose(1, 0, 2)
    up_part = lax.dynamic_update_slice(
        jnp.zeros((nf, ns, q), F32), grad_up_bias.reshape(nf, 1, q), (0, s, 0)
    ).reshape(nf, -1, dl)
    vec_part = jnp.concatenate([vec_part, up_part], axis=1).reshape(nf, vec_rows, wide)
    vec_part = jnp.pad(vec_part, ((0, 0), (0, extra - vec_rows), (0, 0))).astype(BF)
    vec_part = vec_part.reshape(nf * extra, wide)
    qkv_all, vec_sum, out_all = tail_call(nf, ns, grad_qkv, vec_part, grad_out)
    vec_sum = vec_sum[:vec_rows].reshape(-1, dl)
    return (
        output,
        tokens_grad,
        vec_sum[0],
        vec_sum[1],
        qkv_all,
        vec_sum[2],
        vec_sum[3],
        out_all,
        vec_sum[4],
        vec_sum[5],
        vec_sum[6],
        up_all,
        vec_sum[8:].reshape(ffl),
        down_all,
        vec_sum[7],
    )


def solution(mesh):
    rows, cols, vec = P(("fsdp", "seq"), None), P("fsdp", None), P("fsdp")
    return jax.shard_map(
        functools.partial(shards, mesh.shape["fsdp"], mesh.shape["seq"]),
        mesh=mesh,
        in_specs=(rows, rows, cols, cols, vec, vec, cols, vec, vec, cols, vec, vec, vec, cols, vec, cols, vec),
        out_specs=(rows, rows, vec, vec, cols, vec, vec, cols, vec, vec, vec, cols, vec, cols, vec),
        check_vma=False,
    )
```

```python
import functools
import math

import jax
import jax.numpy as jnp
from jax import lax
from jax.experimental import pallas as pl
from jax.experimental.pallas import tpu as pltpu
from jax.sharding import PartitionSpec as P

HEADS = 16
HEAD_DIM = 64
LANES = 128
BF = jnp.bfloat16
F32 = jnp.float32
MASKED = -1e30


def swap(value, axis, size, bit):
    return lax.ppermute(value, axis, [(i, i ^ bit) for i in range(size)])


def falling(size):
    bits = []
    while size > 1:
        size //= 2
        bits.append(size)
    return tuple(bits)


def order_of(bits):
    order = [0]
    for bit in bits:
        order = order + [k ^ bit for k in order]
    return order


def gather_rows(value, axis, size, bits):
    for bit in bits:
        value = jnp.concatenate([value, swap(value, axis, size, bit)], axis=0)
    return value


def scatter_rows(keep, send, axis, size, bits, last=F32):
    for k, bit in enumerate(bits):
        arrived = swap(send, axis, size, bit)
        if k == len(bits) - 1:
            return (keep.astype(F32) + arrived.astype(F32)).astype(last)
        half = keep.shape[0] // 2
        send = (keep[half:].astype(F32) + arrived[half:].astype(F32)).astype(keep.dtype)
        keep = (keep[:half].astype(F32) + arrived[:half].astype(F32)).astype(keep.dtype)


def vmem():
    return pl.BlockSpec(memory_space=pltpu.VMEM)


def smem():
    return pl.BlockSpec(memory_space=pltpu.SMEM)


def whole_call(body, outs, me, *arrays):
    return pl.pallas_call(
        body,
        out_shape=outs,
        in_specs=[smem()] + [vmem()] * len(arrays),
        out_specs=jax.tree.map(lambda _: vmem(), outs),
    )(me.reshape(1).astype(jnp.int32), *arrays)


def remote(src, dst, sems, at, axis, target):
    return pltpu.make_async_remote_copy(
        src_ref=src,
        dst_ref=dst,
        send_sem=sems[0].at[at],
        recv_sem=sems[1].at[at],
        device_id={axis: target},
        device_id_type=pl.DeviceIdType.MESH,
    )


def low_part(size):
    return 2 if size <= 8 else 4


def greet(peers):
    barrier = pltpu.get_barrier_semaphore()
    for axis, target in peers:
        pl.semaphore_signal(
            barrier, inc=1, device_id={axis: target}, device_id_type=pl.DeviceIdType.MESH
        )
    pl.semaphore_wait(barrier, len(peers))


def peers_of(axis, size, lo):
    me = lax.axis_index(axis)
    far = [(axis, me ^ (d * lo)) for d in range(1, size // lo)]
    return far + [(axis, me ^ e) for e in range(1, lo)]


def farthest_first(count):
    return sorted(range(1, count), key=lambda d: -d)


def at_block(ref, index, rows):
    if isinstance(index, int):
        return ref.at[pl.ds(index * rows, rows)]
    return ref.at[pl.ds(pl.multiple_of(index * rows, rows), rows)]


class Gather:
    def __init__(self, src, dst, slot, axis, size, lo, far_sems, near_sems):
        me = lax.axis_index(axis)
        hi, rows = size // lo, src.shape[0]
        self.src, self.dst, self.rows, self.own = src, dst, rows, slot(0, 0, me)
        self.far, self.near = {}, {}
        for d in range(1, hi):
            target = me ^ (d * lo)
            self.far[d] = remote(src, at_block(dst, slot(d, 0, target), rows), far_sems, d - 1, axis, target)
        for d in range(hi):
            origin = src if d == 0 else at_block(dst, slot(d, 0, me), rows)
            for e in range(1, lo):
                target = me ^ e
                self.near[d, e] = remote(
                    origin, at_block(dst, slot(d, e, target), rows), near_sems, d * (lo - 1) + e - 1, axis, target
                )

    def start(self):
        for d in farthest_first(len(self.far) + 1):
            self.far[d].start()
        self.pass_on(0)

    def arrive(self, d):
        self.far[d].wait_recv()
        self.pass_on(d)

    def pass_on(self, d):
        for (at, _), copy in self.near.items():
            if at == d:
                copy.start()

    def arrivals(self):
        return sorted(self.far)

    def finish(self):
        for copy in self.near.values():
            copy.wait_recv()
            copy.wait_send()
        for copy in self.far.values():
            copy.wait_send()


def gather_sems(size, lo, arrays):
    hi = size // lo
    kinds = []
    for _ in range(arrays):
        kinds += [pltpu.SemaphoreType.DMA((max(hi - 1, 1),))] * 2
        kinds += [pltpu.SemaphoreType.DMA((hi * (lo - 1),))] * 2
    return kinds


def head_body(nf, ns, s_order, w, o, v, x, w_all, o_all, v_all, x_all, *sems):
    lf, ls = low_part(nf), 2
    greet(peers_of("fsdp", nf, lf) + peers_of("seq", ns, ls))
    absolute = lambda d, e, me: me ^ (d * lf + e)
    relative = lambda d, e, me: s_order.index(d * ls + e)
    moves = []
    for k, (src, dst) in enumerate([(w, w_all), (v, v_all), (o, o_all)]):
        moves.append(Gather(src, dst, absolute, "fsdp", nf, lf, sems[4 * k : 4 * k + 2], sems[4 * k + 2 : 4 * k + 4]))
    moves.append(Gather(x, x_all, relative, "seq", ns, ls, sems[12:14], sems[14:16]))
    for move in moves:
        move.start()
    me = lax.axis_index("fsdp")
    for src, dst in [(w, w_all), (v, v_all), (o, o_all)]:
        rows = src.shape[0]
        dst[pl.ds(pl.multiple_of(me * rows, rows), rows), :] = src[...]
    x_all[0 : x.shape[0], :] = x[...]
    for d in moves[0].arrivals():
        for move in moves[:3]:
            move.arrive(d)
    for d in moves[3].arrivals():
        moves[3].arrive(d)
    for move in moves:
        move.finish()


def head(nf, ns, s_order, w, o, v, x):
    return pl.pallas_call(
        functools.partial(head_body, nf, ns, s_order),
        out_shape=[
            jax.ShapeDtypeStruct((a.shape[0] * n, a.shape[1]), a.dtype) for a, n in ((w, nf), (o, nf), (v, nf), (x, ns))
        ],
        in_specs=[vmem()] * 4,
        out_specs=[vmem()] * 4,
        scratch_shapes=gather_sems(nf, low_part(nf), 3) + gather_sems(ns, 2, 1),
        compiler_params=pltpu.CompilerParams(collective_id=1, has_side_effects=True),
        name="head",
    )(w, o, v, x)


def tail_body(nf, ns, merged, g, v, o, *rest):
    lf, ls = low_part(nf), 2
    hi = nf // lf
    arrays = [g, v, o]
    rest = list(rest)
    take = lambda count: [rest.pop(0) for _ in range(count)]
    ff = take(merged)
    qkv_out, vec_out, out_out = take(3)
    up_out, down_out = take(2) if merged else (None, None)
    near_in, summed, far_in, mine, everyone = take(3), take(3), take(3), take(3), take(3)
    near_sems, far_sems = [take(2) for _ in arrays], [take(2) for _ in arrays]
    seq_sems = [take(4) for _ in arrays + ff]
    ff_all = take(merged)
    me = lax.axis_index("fsdp")
    greet(peers_of("fsdp", nf, lf) + peers_of("seq", ns, ls))
    relative = lambda d, e, _: d * ls + e
    ff_moves = [
        Gather(a, b, relative, "seq", ns, ls, seq_sems[3][:2], seq_sems[3][2:]) for a, b in zip(ff, ff_all)
    ]
    for move in ff_moves:
        move.start()
    order = farthest_first(hi) + [0]
    rows = [a.shape[0] // nf for a in arrays]
    near, far = {}, {}
    for d in order:
        for e in range(1, lf):
            for k, a in enumerate(arrays):
                at = d * (lf - 1) + e - 1
                near[d, e, k] = remote(
                    at_block(a, me ^ (d * lf + e), rows[k]), near_in[k].at[at], near_sems[k], at, "fsdp", me ^ e
                )
                near[d, e, k].start()
    for d in order:
        for k, a in enumerate(arrays):
            spot = pl.ds(pl.multiple_of((me ^ (d * lf)) * rows[k], rows[k]), rows[k])
            total = a[spot, :].astype(F32)
            for e in range(1, lf):
                near[d, e, k].wait_recv()
                total += near_in[k][d * (lf - 1) + e - 1].astype(F32)
            summed[k][d] = total.astype(BF)
            if d:
                far[d, k] = remote(
                    summed[k].at[d], far_in[k].at[d - 1], far_sems[k], d - 1, "fsdp", me ^ (d * lf)
                )
                far[d, k].start()
    for move in ff_moves:
        for d in move.arrivals():
            move.arrive(d)
    moves = []
    for k, a in enumerate(arrays):
        total = summed[k][0].astype(F32)
        for d in range(1, hi):
            far[d, k].wait_recv()
            total += far_in[k][d - 1].astype(F32)
        mine[k][...] = total.astype(BF)
        moves.append(
            Gather(mine[k], everyone[k], relative, "seq", ns, ls, seq_sems[k][:2], seq_sems[k][2:])
        )
        moves[k].start()
    seq = lax.axis_index("seq")
    for move, a, b in zip(ff_moves, ff, ff_all):
        move.finish()
        q = a.shape[0]
        for r in range(ns):
            here = seq ^ r
            source = a if r == 0 else at_block(b, r, q)
            for c in range(nf):
                spot = pl.multiple_of((c * ns + here) * q, q)
                up_out[:, pl.ds(spot, q)] = source[:, c * q : (c + 1) * q].astype(F32)
            down_out[pl.ds(pl.multiple_of(here * q, q), q), :] = source[:, nf * q :].astype(F32)
    for d in moves[0].arrivals():
        for move in moves:
            move.arrive(d)
    for move in moves:
        move.finish()
    for copy in list(near.values()) + list(far.values()):
        copy.wait_send()
    hl = o.shape[1]
    vec_total = mine[1][...].astype(F32)
    for r in range(ns):
        here = seq ^ r
        sources = [mine[k] if r == 0 else at_block(everyone[k], r, rows[k]) for k in range(3)]
        for c in range(3):
            spot = pl.multiple_of((c * ns + here) * hl, hl)
            qkv_out[:, pl.ds(spot, hl)] = sources[0][:, c * hl : (c + 1) * hl].astype(F32)
        out_out[:, pl.ds(pl.multiple_of(here * hl, hl), hl)] = sources[2][...].astype(F32)
        if r:
            vec_total += sources[1][...].astype(F32)
    vec_out[...] = vec_total


def tail_call(nf, ns, g, v, o, *ff):
    lf = low_part(nf)
    hi = nf // lf
    arrays = [g, v, o]
    blocks = [(a.shape[0] // nf, a.shape[1]) for a in arrays]
    outs = [
        jax.ShapeDtypeStruct((blocks[0][0], ns * g.shape[1]), F32),
        jax.ShapeDtypeStruct(blocks[1], F32),
        jax.ShapeDtypeStruct((blocks[2][0], ns * o.shape[1]), F32),
    ]
    for a in ff:
        q, width = a.shape[0], a.shape[1] - nf * a.shape[0]
        outs += [jax.ShapeDtypeStruct((q, nf * ns * q), F32), jax.ShapeDtypeStruct((ns * q, width), F32)]
    scratch = []
    for lead in (hi * (lf - 1), hi, max(hi - 1, 1)):
        scratch += [pltpu.VMEM((lead,) + b, BF) for b in blocks]
    scratch += [pltpu.VMEM(b, BF) for b in blocks]
    scratch += [pltpu.VMEM((ns * b[0], b[1]), BF) for b in blocks]
    scratch += [pltpu.SemaphoreType.DMA((hi * (lf - 1),))] * 6
    scratch += [pltpu.SemaphoreType.DMA((max(hi - 1, 1),))] * 6
    scratch += gather_sems(ns, 2, 3 + len(ff))
    scratch += [pltpu.VMEM((ns * a.shape[0], a.shape[1]), BF) for a in ff]
    return pl.pallas_call(
        functools.partial(tail_body, nf, ns, len(ff)),
        out_shape=outs,
        in_specs=[vmem()] * (3 + len(ff)),
        out_specs=[vmem()] * len(outs),
        scratch_shapes=scratch,
        compiler_params=pltpu.CompilerParams(collective_id=2, has_side_effects=True),
        name="tail",
    )(g, v, o, *ff)


def place_cols(pieces, me):
    count, (rows, cols) = len(pieces), pieces[0].shape

    def body(me_ref, *refs):
        for r in range(count):
            spot = pl.multiple_of((me_ref[0] ^ r) * cols, cols)
            refs[-1][:, pl.ds(spot, cols)] = refs[r][...]

    return whole_call(
        body, jax.ShapeDtypeStruct((rows, count * cols), pieces[0].dtype), me, *pieces
    )


def take_cols(value, order, groups, me):
    count = len(order)
    rows, cols = value.shape[0], value.shape[1] // count
    each = count // groups

    def body(me_ref, src, *outs):
        for k, r in enumerate(order):
            spot = pl.multiple_of((me_ref[0] ^ r) * cols, cols)
            base = (k % each) * rows
            outs[k // each][base : base + rows, :] = src[:, pl.ds(spot, cols)]

    return whole_call(
        body, [jax.ShapeDtypeStruct((each * rows, cols), value.dtype)] * groups, me, value
    )


def spread_cols(stacked, order, first, last, sections, me, kind=F32):
    count = len(order)
    rows = stacked.shape[0] // count
    cols = (last - first) // sections
    if cols % LANES:
        blocks = stacked.reshape(count, rows, -1)[:, :, first:last]
        blocks = blocks[jnp.argsort(jnp.array(order) ^ me)].reshape(count, rows, sections, cols)
        return blocks.transpose(1, 2, 0, 3).reshape(rows, -1).astype(kind)

    def body(me_ref, src, out):
        for k, r in enumerate(order):
            here = me_ref[0] ^ r
            for c in range(sections):
                spot = pl.multiple_of((c * count + here) * cols, cols)
                out[:, pl.ds(spot, cols)] = src[
                    k * rows : (k + 1) * rows, first + c * cols : first + (c + 1) * cols
                ].astype(kind)

    return whole_call(
        body, jax.ShapeDtypeStruct((rows, count * sections * cols), kind), me, stacked
    )


def spread_rows(stacked, order, first, last, me):
    count = len(order)
    rows = stacked.shape[0] // count

    def body(me_ref, src, out):
        for k, r in enumerate(order):
            spot = pl.multiple_of((me_ref[0] ^ r) * rows, rows)
            out[pl.ds(spot, rows), :] = src[k * rows : (k + 1) * rows, first:last].astype(F32)

    return whole_call(
        body, jax.ShapeDtypeStruct((count * rows, last - first), F32), me, stacked
    )


def pair_mask(shape, head):
    lane = lax.broadcasted_iota(jnp.int32, shape, 1)
    return (lane >= head * HEAD_DIM) & (lane < (head + 1) * HEAD_DIM)


def dot_nt(a, b):
    return lax.dot_general(a, b, (((1,), (1,)), ((), ())), preferred_element_type=F32)


def dot_nn(a, b):
    return lax.dot_general(a, b, (((1,), (0,)), ((), ())), preferred_element_type=F32)


def dot_tn(a, b):
    return lax.dot_general(a, b, (((0,), (0,)), ((), ())), preferred_element_type=F32)


def row_starts(ends_ref, count, row_at, block):
    row = lax.broadcasted_iota(jnp.int32, (1, block), 1) + row_at
    start = jnp.zeros((1, block), jnp.int32)
    for k in range(count):
        start = jnp.where(row >= ends_ref[k], ends_ref[k], start)
    return start


def start_of(ends_ref, count, row):
    start = jnp.int32(0)
    for k in range(count):
        start = jnp.where(row >= ends_ref[k], ends_ref[k], start)
    return start


def over_tiles(ends_ref, count, row_at, block, span, tile):
    start_row = row_starts(ends_ref, count, row_at, block)
    key = lax.broadcasted_iota(jnp.int32, (span, block), 0)
    apart = (key - lax.broadcasted_iota(jnp.int32, (span, block), 1)).astype(F32)
    last = start_of(ends_ref, count, row_at + block - 1)

    def one(j, _):
        at = pl.multiple_of(j * span, span)
        dist = apart + (at - row_at).astype(F32)
        inner = (at >= last) & (at + span <= row_at)

        @pl.when(inner)
        def _():
            tile(at, dist)

        @pl.when(jnp.logical_not(inner))
        def _():
            tile(at, jnp.where((dist <= 0) & (key + at >= start_row), dist, MASKED))

        return 0

    low = lax.div(start_of(ends_ref, count, row_at), span)
    lax.fori_loop(low, lax.div(row_at + block, span), one, 0)


def pair_slice(p):
    return slice(p * LANES, (p + 1) * LANES)


def attend_body(block, span, pairs, count, ends_ref, slope_ref, q_ref, k_ref, v_ref, o_ref, lse_ref, m_ref, l_ref, acc_ref):
    row_at = pl.program_id(0) * block
    m_ref[...] = jnp.full_like(m_ref, -3e38)
    l_ref[...] = jnp.zeros_like(l_ref)
    acc_ref[...] = jnp.zeros_like(acc_ref)
    heads = []
    for p in range(pairs):
        queries = q_ref[:, pair_slice(p)]
        heads += [jnp.where(pair_mask(queries.shape, h), queries, 0).astype(BF) for h in range(2)]

    def tile(at, dist):
        for p in range(pairs):
            keys = k_ref[pl.ds(at, span), pair_slice(p)]
            values = v_ref[pl.ds(at, span), pair_slice(p)].T
            for side in range(2):
                h, half = 2 * p + side, slice(side * HEAD_DIM, (side + 1) * HEAD_DIM)
                scores = dot_nt(keys, heads[h]) + slope_ref[h] * dist
                old = m_ref[h : h + 1, :]
                new = jnp.maximum(old, jnp.max(scores, axis=0, keepdims=True))
                shrink = jnp.exp(old - new)
                weight = jnp.exp(scores - new)
                m_ref[h : h + 1, :] = new
                l_ref[h : h + 1, :] = l_ref[h : h + 1, :] * shrink + jnp.sum(
                    weight, axis=0, keepdims=True
                )
                acc_ref[p, half] = acc_ref[p, half] * shrink + dot_nn(
                    values[half], weight.astype(BF)
                )

    over_tiles(ends_ref, count, row_at, block, span, tile)
    for p in range(pairs):
        top = acc_ref[p, :HEAD_DIM] / l_ref[2 * p : 2 * p + 1, :]
        bottom = acc_ref[p, HEAD_DIM:] / l_ref[2 * p + 1 : 2 * p + 2, :]
        o_ref[:, pair_slice(p)] = jnp.concatenate([top, bottom], axis=0).T.astype(BF)
    lse_ref[...] = m_ref[...] + jnp.log(l_ref[...])


def attend(qkv, ends, slopes, block, span):
    rows, width = qkv.shape[0], qkv.shape[1] // 3
    pairs = width // LANES
    return pl.pallas_call(
        functools.partial(attend_body, block, span, pairs, ends.shape[0]),
        out_shape=(
            jax.ShapeDtypeStruct((rows, width), BF),
            jax.ShapeDtypeStruct((2 * pairs, rows), F32),
        ),
        grid=(rows // block,),
        in_specs=[
            smem(),
            smem(),
            pl.BlockSpec((block, width), lambda i: (i, 0)),
            pl.BlockSpec((rows, width), lambda i: (0, 1)),
            pl.BlockSpec((rows, width), lambda i: (0, 2)),
        ],
        out_specs=(
            pl.BlockSpec((block, width), lambda i: (i, 0)),
            pl.BlockSpec((2 * pairs, block), lambda i: (0, i)),
        ),
        scratch_shapes=[
            pltpu.VMEM((2 * pairs, block), F32),
            pltpu.VMEM((2 * pairs, block), F32),
            pltpu.VMEM((pairs, LANES, block), F32),
        ],
        cost_estimate=pl.CostEstimate(
            flops=4 * rows * rows * width, bytes_accessed=10 * rows * width, transcendentals=rows * rows
        ),
        name="attend",
    )(ends, slopes, qkv, qkv, qkv)


def attend_back_body(
    block, span, pairs, count, ends_ref, slope_ref, lse_ref, q_ref, k_ref, v_ref, o_ref, g_ref, d_ref, dq_acc, dk_acc, dv_acc
):
    row_at = pl.multiple_of(pl.program_id(0) * block, block)
    width = pairs * LANES

    @pl.when(pl.program_id(0) == 0)
    def _():
        dk_acc[...] = jnp.zeros_like(dk_acc)
        dv_acc[...] = jnp.zeros_like(dv_acc)

    dq_acc[...] = jnp.zeros_like(dq_acc)
    q_heads, g_heads, dots = [], [], []
    for p in range(pairs):
        queries, grads = q_ref[:, pair_slice(p)], g_ref[:, pair_slice(p)]
        product = (o_ref[:, pair_slice(p)].astype(F32) * grads.astype(F32)).T
        for side in range(2):
            mask = pair_mask(queries.shape, side)
            half = slice(side * HEAD_DIM, (side + 1) * HEAD_DIM)
            q_heads.append(jnp.where(mask, queries, 0).astype(BF))
            g_heads.append(jnp.where(mask, grads, 0).astype(BF))
            dots.append(jnp.sum(product[half], axis=0, keepdims=True))

    def tile(at, dist):
        for p in range(pairs):
            keys = k_ref[pl.ds(at, span), pair_slice(p)]
            values = v_ref[pl.ds(at, span), pair_slice(p)]
            turned = keys.T
            dv, dk = [], []
            for side in range(2):
                h = 2 * p + side
                scores = dot_nt(keys, q_heads[h]) + slope_ref[h] * dist
                prob = jnp.exp(scores - lse_ref[h : h + 1, :])
                dscore = (prob * (dot_nt(values, g_heads[h]) - dots[h])).astype(BF)
                dv.append(dot_nn(prob.astype(BF), g_heads[h]))
                dk.append(dot_nn(dscore, q_heads[h]))
                rows = slice(h * HEAD_DIM, (h + 1) * HEAD_DIM)
                half = slice(side * HEAD_DIM, (side + 1) * HEAD_DIM)
                dq_acc[rows] += dot_nn(turned[half], dscore)
            dv_acc[pl.ds(at, span), pair_slice(p)] += dv[0] + dv[1]
            dk_acc[pl.ds(at, span), pair_slice(p)] += dk[0] + dk[1]

    over_tiles(ends_ref, count, row_at, block, span, tile)
    d_ref[pl.ds(row_at, block), 0:width] = (dq_acc[...].T * (1.0 / math.sqrt(HEAD_DIM))).astype(BF)

    @pl.when(pl.program_id(0) == pl.num_programs(0) - 1)
    def _():
        d_ref[:, width : 2 * width] = dk_acc[...].astype(BF)
        d_ref[:, 2 * width :] = dv_acc[...].astype(BF)


def attend_back(qkv, out, grad, lse, ends, slopes, block, span):
    rows, width = qkv.shape[0], qkv.shape[1] // 3
    pairs = width // LANES
    return pl.pallas_call(
        functools.partial(attend_back_body, block, span, pairs, ends.shape[0]),
        out_shape=jax.ShapeDtypeStruct((rows, 3 * width), BF),
        grid=(rows // block,),
        in_specs=[
            smem(),
            smem(),
            pl.BlockSpec((2 * pairs, block), lambda i: (0, i)),
            pl.BlockSpec((block, width), lambda i: (i, 0)),
            pl.BlockSpec((rows, width), lambda i: (0, 1)),
            pl.BlockSpec((rows, width), lambda i: (0, 2)),
            pl.BlockSpec((block, width), lambda i: (i, 0)),
            pl.BlockSpec((block, width), lambda i: (i, 0)),
        ],
        out_specs=pl.BlockSpec((rows, 3 * width), lambda i: (0, 0)),
        scratch_shapes=[
            pltpu.VMEM((width, block), F32),
            pltpu.VMEM((rows, width), F32),
            pltpu.VMEM((rows, width), F32),
        ],
        cost_estimate=pl.CostEstimate(
            flops=10 * rows * rows * width, bytes_accessed=20 * rows * width, transcendentals=rows * rows
        ),
        name="attend_back",
    )(ends, slopes, lse, qkv, qkv, qkv, out, grad)


def normalize(values):
    average = jnp.mean(values, axis=-1, keepdims=True)
    centered = values - average
    variance = jnp.mean(centered * centered, axis=-1, keepdims=True)
    scale = lax.rsqrt(variance + 1e-05)
    return centered * scale, scale


def norm_back(grad, gain, normed, scale):
    e = grad * gain
    return scale * (
        e
        - jnp.mean(e, axis=-1, keepdims=True)
        - normed * jnp.mean(e * normed, axis=-1, keepdims=True)
    )


def gelu_and_slope(v):
    c = math.sqrt(2 / math.pi)
    t = jnp.tanh(c * (v + 0.044715 * v * v * v))
    slope = 0.5 * (1 + t) + 0.5 * v * (1 - t * t) * c * (1 + 3 * 0.044715 * v * v)
    return 0.5 * v * (1 + t), slope


def mm(a, b):
    return jnp.dot(a, b, preferred_element_type=F32)


def mm_nt(a, b):
    return lax.dot_general(a, b, (((1,), (1,)), ((), ())), preferred_element_type=F32)


def mm_tn(a, b):
    return lax.dot_general(a, b, (((0,), (0,)), ((), ())), preferred_element_type=F32)


def shards(
    nf,
    ns,
    tokens,
    cotangent,
    seq_lengths,
    stream_order,
    first_gain,
    first_shift,
    qkv_weight,
    query_bias,
    value_bias,
    out_weight,
    out_bias,
    second_gain,
    second_shift,
    up_weight,
    up_bias,
    down_weight,
    down_bias,
):
    f, s = lax.axis_index("fsdp"), lax.axis_index("seq")
    toks, width = tokens.shape
    group = toks * ns
    dl, hl = width // nf, width // ns
    ff = up_weight.shape[1]
    ffl = ff // nf
    q = ffl // ns
    ffs = nf * q
    wide = 3 * hl
    bits_s = falling(ns)
    s_order = order_of(bits_s)
    back = lambda bits: tuple(reversed(bits))

    vectors = jnp.concatenate(
        [first_gain, first_shift, query_bias, value_bias, out_bias, second_gain, second_shift, down_bias, up_bias]
    )
    vec_rows = vectors.shape[0] // wide
    extra = 16
    qkv_shard = jnp.concatenate(
        [lax.dynamic_slice(qkv_weight, (0, k * width + s * hl), (dl, hl)) for k in range(3)], axis=1
    )
    vec_shard = jnp.pad(vectors.reshape(vec_rows, wide), ((0, extra - vec_rows), (0, 0)))
    out_shard = lax.dynamic_slice(out_weight, (0, s * hl), (dl, hl))
    qkv_full, out_cols, vec_all, x_all = head(nf, ns, s_order, qkv_shard, out_shard, vec_shard, tokens)
    up_shard = lax.dynamic_index_in_dim(
        up_weight.reshape(dl, nf, ns, q), s, 2, keepdims=False
    ).reshape(dl, ffs)
    down_shard = lax.dynamic_slice(down_weight, (s * q, 0), (q, width))
    merged = q == dl and q % LANES == 0

    if merged:
        packed = jnp.concatenate([up_shard, down_shard], axis=1)
        packed, cotangent, qkv_full = lax.optimization_barrier((packed, cotangent, qkv_full))
        packed = lax.all_gather(packed, "fsdp", axis=0, tiled=True)
        up_full, down_full = packed[:, :ffs], packed[:, ffs:]
    else:
        up_shard, down_shard, cotangent, qkv_full = lax.optimization_barrier(
            (up_shard, down_shard, cotangent, qkv_full)
        )
        up_full = lax.all_gather(up_shard, "fsdp", axis=0, tiled=True)
        down_full = lax.all_gather(down_shard, "fsdp", axis=0, tiled=True)
    near = bits_s[-1:]
    far = bits_s[:-1]
    out_full = spread_cols(gather_rows(out_cols, "seq", ns, bits_s), s_order, 0, hl, 1, s, BF)
    ct_near = gather_rows(cotangent, "seq", ns, near)
    ct_far = gather_rows(cotangent, "seq", ns, far)[toks:]
    ct_far = gather_rows(ct_far, "seq", ns, near)

    vecs = vec_all.reshape(nf, extra, wide)[:, :vec_rows].reshape(nf, -1, dl).astype(F32)
    full = vecs[:, :8].transpose(1, 0, 2).reshape(8, width)
    gain_one, shift_one, bias_query, bias_value, bias_out, gain_two, shift_two, bias_down = full
    bias_up = lax.dynamic_index_in_dim(vecs[:, 8:].reshape(nf, ns, q), s, 1, keepdims=False)
    bias_up = bias_up.reshape(ffs)
    bias_qkv = jnp.concatenate(
        [
            lax.dynamic_slice(bias_query, (s * hl,), (hl,)),
            jnp.zeros((hl,), F32),
            lax.dynamic_slice(bias_value, (s * hl,), (hl,)),
        ]
    )
    query_scale = jnp.where(jnp.arange(wide) < hl, 1.0 / math.sqrt(HEAD_DIM), 1.0)

    positions = stream_order[0].reshape(ns, toks)[jnp.array(s_order) ^ s].reshape(group)
    ends = jnp.cumsum(seq_lengths[0])
    line = jnp.arange(group)
    block, span = min(512, group), min(512, group)
    ends = ends.astype(jnp.int32)
    heads_here = hl // HEAD_DIM
    slopes = jnp.exp2(
        -(s * heads_here + 1 + jnp.arange(heads_here)).astype(F32) * (8.0 / HEADS)
    )
    to_sorted = (positions[None, :] == line[:, None]).astype(BF)

    n_all, _ = normalize(x_all.astype(F32))
    a_all = (n_all * gain_one + shift_one).astype(BF)
    qkv = ((mm(a_all, qkv_full) + bias_qkv).astype(BF).astype(F32) * query_scale).astype(BF)
    qkv_sorted = mm(to_sorted, qkv).astype(BF)
    o_sorted, lse = attend(qkv_sorted, ends, slopes, block, span)
    context_heads = mm_tn(to_sorted, o_sorted).astype(BF)

    def exchange(blocks):
        return [blocks[0]] + [swap(blocks[r], "seq", ns, r) for r in range(1, ns)]

    context = place_cols(
        exchange([context_heads[k * toks : (k + 1) * toks] for k in (s_order.index(r) for r in range(ns))]), s
    )

    x_own = tokens.astype(F32)
    residual = x_own + mm(context, out_full) + bias_out
    n_two, scale_two = normalize(residual)
    m_low = (n_two * gain_two + shift_two).astype(BF)
    m_far = gather_rows(m_low, "seq", ns, far)[toks:]
    m_near = gather_rows(m_low, "seq", ns, near)
    m_far = gather_rows(m_far, "seq", ns, near)

    def feed_forward(m, ct):
        activated, slope = gelu_and_slope(mm(m, up_full) + bias_up)
        act = activated.astype(BF)
        d_pre = (mm_nt(ct, down_full) * slope).astype(BF)
        return act, d_pre, mm_nt(d_pre, up_full).astype(BF)

    act_near, d_pre_near, d_m_near = feed_forward(m_near, ct_near)
    act_far, d_pre_far, d_m_far = feed_forward(m_far, ct_far)

    def home_near(near_part, far_part):
        half = far_part.shape[0] // 2
        keep_near = near_part[:toks].astype(F32) + swap(near_part[toks:], "seq", ns, near[0]).astype(F32)
        keep_far = far_part[:half].astype(F32) + swap(far_part[half:], "seq", ns, near[0]).astype(F32)
        return keep_near, keep_far.astype(BF)

    def home_far(keep_near, keep_far):
        blocks = dict(zip(order_of(far)[1:], jnp.split(keep_far, ns // 2 - 1)))
        blocks[0] = keep_near
        for bit in back(far):
            for r in sorted(blocks):
                if r & bit:
                    arrived = swap(blocks.pop(r).astype(BF), "seq", ns, bit)
                    blocks[r ^ bit] = blocks[r ^ bit].astype(F32) + arrived.astype(F32)
        return blocks[0]

    d_m = home_far(*home_near(d_m_near, d_m_far))
    total_near, total_far = home_near(mm(act_near, down_full).astype(BF), mm(act_far, down_full).astype(BF))
    grad_up = (mm_tn(m_near, d_pre_near) + mm_tn(m_far, d_pre_far)).astype(BF)
    grad_down = (mm_tn(act_near, ct_near) + mm_tn(act_far, ct_far)).astype(BF)
    grad_up_bias = jnp.sum(d_pre_near, axis=0, dtype=F32) + jnp.sum(d_pre_far, axis=0, dtype=F32)

    def scatter_whole(value):
        return lax.psum_scatter(value, "fsdp", scatter_dimension=0, tiled=True)

    if merged:
        grad_ff = [scatter_whole(jnp.concatenate([grad_up, grad_down], axis=1))]
    else:
        grad_ff = []
        grad_up = gather_rows(scatter_whole(grad_up), "seq", ns, bits_s)
        grad_down = gather_rows(scatter_whole(grad_down), "seq", ns, bits_s)
        up_all = spread_cols(grad_up, s_order, 0, ffs, nf, s)
        down_all = spread_rows(grad_down, s_order, 0, width, s)

    ct_own = cotangent.astype(F32)
    grad_down_bias = jnp.sum(ct_own, axis=0)
    grad_gain_two = jnp.sum(d_m * n_two, axis=0)
    grad_shift_two = jnp.sum(d_m, axis=0)
    d_res = ct_own + norm_back(d_m, gain_two, n_two, scale_two)
    d_att = d_res.astype(BF)
    grad_out_bias = jnp.sum(d_att, axis=0, dtype=F32)
    d_context = exchange(take_cols(mm_nt(d_att, out_full).astype(BF), list(range(ns)), ns, s))
    d_context = jnp.concatenate([d_context[r] for r in s_order], axis=0)
    total_near, total_far, d_context = lax.optimization_barrier((total_near, total_far, d_context))
    output = (residual + home_far(total_near, total_far) + bias_down).astype(BF)
    d_o_sorted = mm(to_sorted, d_context).astype(BF)
    grad_out = take_cols(mm_tn(context, d_att).astype(BF), s_order, 2, s)
    grad_out = scatter_rows(*grad_out, "seq", ns, back(bits_s), BF)

    d_qkv_sorted = attend_back(
        qkv_sorted, o_sorted, d_o_sorted, lse, ends, slopes, block, span // 2
    )
    d_qkv_sorted, output, grad_out = lax.optimization_barrier((d_qkv_sorted, output, grad_out))
    d_qkv = mm_tn(to_sorted, d_qkv_sorted).astype(BF)
    d_a_part = mm_nt(d_qkv, qkv_full)
    d_a_low = d_a_part.astype(BF)
    d_a = scatter_rows(d_a_low[: group // 2], d_a_low[group // 2 :], "seq", ns, back(bits_s))
    grad_qkv = mm_tn(a_all, d_qkv).astype(BF)
    grad_bias_qkv = jnp.sum(d_qkv, axis=0, dtype=F32)
    grad_gain_one = jnp.sum(d_a_part * n_all, axis=0)
    grad_shift_one = jnp.sum(d_a_part, axis=0)
    n_own, scale_own = normalize(x_own)
    tokens_grad = d_res + norm_back(d_a, gain_one, n_own, scale_own)

    def spread(part):
        return lax.dynamic_update_slice(jnp.zeros((width,), F32), part, (s * hl,))

    vec_part = jnp.stack(
        [
            grad_gain_one,
            grad_shift_one,
            spread(grad_bias_qkv[:hl]),
            spread(grad_bias_qkv[2 * hl :]),
            grad_out_bias,
            grad_gain_two,
            grad_shift_two,
            grad_down_bias,
        ]
    )
    vec_part = vec_part.reshape(8, nf, dl).transpose(1, 0, 2)
    up_part = lax.dynamic_update_slice(
        jnp.zeros((nf, ns, q), F32), grad_up_bias.reshape(nf, 1, q), (0, s, 0)
    ).reshape(nf, -1, dl)
    vec_part = jnp.concatenate([vec_part, up_part], axis=1).reshape(nf, vec_rows, wide)
    vec_part = jnp.pad(vec_part, ((0, 0), (0, extra - vec_rows), (0, 0))).astype(BF)
    vec_part = vec_part.reshape(nf * extra, wide)
    qkv_all, vec_sum, out_all, *ff_all = tail_call(nf, ns, grad_qkv, vec_part, grad_out, *grad_ff)
    if merged:
        up_all, down_all = ff_all
    vec_sum = vec_sum[:vec_rows].reshape(-1, dl)
    return (
        output,
        tokens_grad,
        vec_sum[0],
        vec_sum[1],
        qkv_all,
        vec_sum[2],
        vec_sum[3],
        out_all,
        vec_sum[4],
        vec_sum[5],
        vec_sum[6],
        up_all,
        vec_sum[8:].reshape(ffl),
        down_all,
        vec_sum[7],
    )


def solution(mesh):
    rows, cols, vec = P(("fsdp", "seq"), None), P("fsdp", None), P("fsdp")
    return jax.shard_map(
        functools.partial(shards, mesh.shape["fsdp"], mesh.shape["seq"]),
        mesh=mesh,
        in_specs=(rows, rows, cols, cols, vec, vec, cols, vec, vec, cols, vec, vec, vec, cols, vec, cols, vec),
        out_specs=(rows, rows, vec, vec, cols, vec, vec, cols, vec, vec, vec, cols, vec, cols, vec),
        check_vma=False,
    )
```

```python
import functools
import math

import jax
import jax.numpy as jnp
from jax import lax
from jax.experimental import pallas as pl
from jax.experimental.pallas import tpu as pltpu
from jax.sharding import PartitionSpec as P

HEADS = 16
HEAD_DIM = 64
LANES = 128
BF = jnp.bfloat16
F32 = jnp.float32
MASKED = -1e30


def swap(value, axis, size, bit):
    return lax.ppermute(value, axis, [(i, i ^ bit) for i in range(size)])


def falling(size):
    bits = []
    while size > 1:
        size //= 2
        bits.append(size)
    return tuple(bits)


def order_of(bits):
    order = [0]
    for bit in bits:
        order = order + [k ^ bit for k in order]
    return order


def gather_rows(value, axis, size, bits):
    for bit in bits:
        value = jnp.concatenate([value, swap(value, axis, size, bit)], axis=0)
    return value


def scatter_rows(keep, send, axis, size, bits, last=F32):
    for k, bit in enumerate(bits):
        arrived = swap(send, axis, size, bit)
        if k == len(bits) - 1 and last is None:
            return keep, arrived
        if k == len(bits) - 1:
            return (keep.astype(F32) + arrived.astype(F32)).astype(last)
        half = keep.shape[0] // 2
        send = (keep[half:].astype(F32) + arrived[half:].astype(F32)).astype(keep.dtype)
        keep = (keep[:half].astype(F32) + arrived[:half].astype(F32)).astype(keep.dtype)


def vmem():
    return pl.BlockSpec(memory_space=pltpu.VMEM)


def smem():
    return pl.BlockSpec(memory_space=pltpu.SMEM)


def whole_call(body, outs, me, *arrays):
    return pl.pallas_call(
        body,
        out_shape=outs,
        in_specs=[smem()] + [vmem()] * len(arrays),
        out_specs=jax.tree.map(lambda _: vmem(), outs),
    )(me.reshape(1).astype(jnp.int32), *arrays)


def remote(src, dst, sems, at, axis, target):
    return pltpu.make_async_remote_copy(
        src_ref=src,
        dst_ref=dst,
        send_sem=sems[0].at[at],
        recv_sem=sems[1].at[at],
        device_id={axis: target},
        device_id_type=pl.DeviceIdType.MESH,
    )


def low_part(size):
    return 2 if size <= 8 else 4


def greet(peers):
    barrier = pltpu.get_barrier_semaphore()
    for axis, target in peers:
        pl.semaphore_signal(
            barrier, inc=1, device_id={axis: target}, device_id_type=pl.DeviceIdType.MESH
        )
    pl.semaphore_wait(barrier, len(peers))


def peers_of(axis, size, lo):
    me = lax.axis_index(axis)
    far = [(axis, me ^ (d * lo)) for d in range(1, size // lo)]
    return far + [(axis, me ^ e) for e in range(1, lo)]


def farthest_first(count):
    return sorted(range(1, count), key=lambda d: -d)


def at_block(ref, index, rows):
    if isinstance(index, int):
        return ref.at[pl.ds(index * rows, rows)]
    return ref.at[pl.ds(pl.multiple_of(index * rows, rows), rows)]


class Gather:
    def __init__(self, src, dst, slot, axis, size, lo, far_sems, near_sems):
        me = lax.axis_index(axis)
        hi, rows = size // lo, src.shape[0]
        self.src, self.dst, self.rows, self.own = src, dst, rows, slot(0, 0, me)
        self.far, self.near = {}, {}
        for d in range(1, hi):
            target = me ^ (d * lo)
            self.far[d] = remote(src, at_block(dst, slot(d, 0, target), rows), far_sems, d - 1, axis, target)
        for d in range(hi):
            origin = src if d == 0 else at_block(dst, slot(d, 0, me), rows)
            for e in range(1, lo):
                target = me ^ e
                self.near[d, e] = remote(
                    origin, at_block(dst, slot(d, e, target), rows), near_sems, d * (lo - 1) + e - 1, axis, target
                )

    def start(self):
        for d in farthest_first(len(self.far) + 1):
            self.far[d].start()
        self.pass_on(0)

    def arrive(self, d):
        self.far[d].wait_recv()
        self.pass_on(d)

    def pass_on(self, d):
        for (at, _), copy in self.near.items():
            if at == d:
                copy.start()

    def arrivals(self):
        return sorted(self.far)

    def finish(self):
        for copy in self.near.values():
            copy.wait_recv()
            copy.wait_send()
        for copy in self.far.values():
            copy.wait_send()


def gather_sems(size, lo, arrays):
    hi = size // lo
    kinds = []
    for _ in range(arrays):
        kinds += [pltpu.SemaphoreType.DMA((max(hi - 1, 1),))] * 2
        kinds += [pltpu.SemaphoreType.DMA((hi * (lo - 1),))] * 2
    return kinds


def head_body(nf, ns, s_order, w, o, v, x, w_all, o_all, v_all, x_all, *sems):
    lf, ls = low_part(nf), 2
    greet(peers_of("fsdp", nf, lf) + peers_of("seq", ns, ls))
    absolute = lambda d, e, me: me ^ (d * lf + e)
    relative = lambda d, e, me: s_order.index(d * ls + e)
    moves = []
    for k, (src, dst) in enumerate([(w, w_all), (v, v_all), (o, o_all)]):
        moves.append(Gather(src, dst, absolute, "fsdp", nf, lf, sems[4 * k : 4 * k + 2], sems[4 * k + 2 : 4 * k + 4]))
    moves.append(Gather(x, x_all, relative, "seq", ns, ls, sems[12:14], sems[14:16]))
    for move in moves:
        move.start()
    me = lax.axis_index("fsdp")
    for src, dst in [(w, w_all), (v, v_all), (o, o_all)]:
        rows = src.shape[0]
        dst[pl.ds(pl.multiple_of(me * rows, rows), rows), :] = src[...]
    x_all[0 : x.shape[0], :] = x[...]
    for d in moves[0].arrivals():
        for move in moves[:3]:
            move.arrive(d)
    for d in moves[3].arrivals():
        moves[3].arrive(d)
    for move in moves:
        move.finish()


def head(nf, ns, s_order, w, o, v, x):
    return pl.pallas_call(
        functools.partial(head_body, nf, ns, s_order),
        out_shape=[
            jax.ShapeDtypeStruct((a.shape[0] * n, a.shape[1]), a.dtype) for a, n in ((w, nf), (o, nf), (v, nf), (x, ns))
        ],
        in_specs=[vmem()] * 4,
        out_specs=[vmem()] * 4,
        scratch_shapes=gather_sems(nf, low_part(nf), 3) + gather_sems(ns, 2, 1),
        compiler_params=pltpu.CompilerParams(collective_id=1, has_side_effects=True),
        name="head",
    )(w, o, v, x)


def tail_body(nf, ns, merged, g, v, o, *rest):
    lf, ls = low_part(nf), 2
    hi = nf // lf
    arrays = [g, v, o]
    rest = list(rest)
    take = lambda count: [rest.pop(0) for _ in range(count)]
    ff = take(merged)
    qkv_out, vec_out, out_out = take(3)
    up_out, down_out = take(2) if merged else (None, None)
    near_in, summed, far_in, mine, everyone = take(3), take(3), take(3), take(3), take(3)
    near_sems, far_sems = [take(2) for _ in arrays], [take(2) for _ in arrays]
    seq_sems = [take(4) for _ in arrays + ff]
    ff_all = take(merged)
    me = lax.axis_index("fsdp")
    greet(peers_of("fsdp", nf, lf) + peers_of("seq", ns, ls))
    relative = lambda d, e, _: d * ls + e
    ff_moves = [
        Gather(a, b, relative, "seq", ns, ls, seq_sems[3][:2], seq_sems[3][2:]) for a, b in zip(ff, ff_all)
    ]
    for move in ff_moves:
        move.start()
    order = farthest_first(hi) + [0]
    rows = [a.shape[0] // nf for a in arrays]
    near, far = {}, {}
    for d in order:
        for e in range(1, lf):
            for k, a in enumerate(arrays):
                at = d * (lf - 1) + e - 1
                near[d, e, k] = remote(
                    at_block(a, me ^ (d * lf + e), rows[k]), near_in[k].at[at], near_sems[k], at, "fsdp", me ^ e
                )
                near[d, e, k].start()
    for d in order:
        for k, a in enumerate(arrays):
            spot = pl.ds(pl.multiple_of((me ^ (d * lf)) * rows[k], rows[k]), rows[k])
            total = a[spot, :].astype(F32)
            for e in range(1, lf):
                near[d, e, k].wait_recv()
                total += near_in[k][d * (lf - 1) + e - 1].astype(F32)
            summed[k][d] = total.astype(BF)
            if d:
                far[d, k] = remote(
                    summed[k].at[d], far_in[k].at[d - 1], far_sems[k], d - 1, "fsdp", me ^ (d * lf)
                )
                far[d, k].start()
    for move in ff_moves:
        for d in move.arrivals():
            move.arrive(d)
    moves = []
    for k, a in enumerate(arrays):
        total = summed[k][0].astype(F32)
        for d in range(1, hi):
            far[d, k].wait_recv()
            total += far_in[k][d - 1].astype(F32)
        mine[k][...] = total.astype(BF)
        moves.append(
            Gather(mine[k], everyone[k], relative, "seq", ns, ls, seq_sems[k][:2], seq_sems[k][2:])
        )
        moves[k].start()
    seq = lax.axis_index("seq")
    for move, a, b in zip(ff_moves, ff, ff_all):
        move.finish()
        q = a.shape[0]
        for r in range(ns):
            here = seq ^ r
            source = a if r == 0 else at_block(b, r, q)
            for c in range(nf):
                spot = pl.multiple_of((c * ns + here) * q, q)
                up_out[:, pl.ds(spot, q)] = source[:, c * q : (c + 1) * q].astype(F32)
            down_out[pl.ds(pl.multiple_of(here * q, q), q), :] = source[:, nf * q :].astype(F32)
    for d in moves[0].arrivals():
        for move in moves:
            move.arrive(d)
    for move in moves:
        move.finish()
    for copy in list(near.values()) + list(far.values()):
        copy.wait_send()
    hl = o.shape[1]
    vec_total = mine[1][...].astype(F32)
    for r in range(ns):
        here = seq ^ r
        sources = [mine[k] if r == 0 else at_block(everyone[k], r, rows[k]) for k in range(3)]
        for c in range(3):
            spot = pl.multiple_of((c * ns + here) * hl, hl)
            qkv_out[:, pl.ds(spot, hl)] = sources[0][:, c * hl : (c + 1) * hl].astype(F32)
        out_out[:, pl.ds(pl.multiple_of(here * hl, hl), hl)] = sources[2][...].astype(F32)
        if r:
            vec_total += sources[1][...].astype(F32)
    vec_out[...] = vec_total


def tail_call(nf, ns, g, v, o, *ff):
    lf = low_part(nf)
    hi = nf // lf
    arrays = [g, v, o]
    blocks = [(a.shape[0] // nf, a.shape[1]) for a in arrays]
    outs = [
        jax.ShapeDtypeStruct((blocks[0][0], ns * g.shape[1]), F32),
        jax.ShapeDtypeStruct(blocks[1], F32),
        jax.ShapeDtypeStruct((blocks[2][0], ns * o.shape[1]), F32),
    ]
    for a in ff:
        q, width = a.shape[0], a.shape[1] - nf * a.shape[0]
        outs += [jax.ShapeDtypeStruct((q, nf * ns * q), F32), jax.ShapeDtypeStruct((ns * q, width), F32)]
    scratch = []
    for lead in (hi * (lf - 1), hi, max(hi - 1, 1)):
        scratch += [pltpu.VMEM((lead,) + b, BF) for b in blocks]
    scratch += [pltpu.VMEM(b, BF) for b in blocks]
    scratch += [pltpu.VMEM((ns * b[0], b[1]), BF) for b in blocks]
    scratch += [pltpu.SemaphoreType.DMA((hi * (lf - 1),))] * 6
    scratch += [pltpu.SemaphoreType.DMA((max(hi - 1, 1),))] * 6
    scratch += gather_sems(ns, 2, 3 + len(ff))
    scratch += [pltpu.VMEM((ns * a.shape[0], a.shape[1]), BF) for a in ff]
    return pl.pallas_call(
        functools.partial(tail_body, nf, ns, len(ff)),
        out_shape=outs,
        in_specs=[vmem()] * (3 + len(ff)),
        out_specs=[vmem()] * len(outs),
        scratch_shapes=scratch,
        compiler_params=pltpu.CompilerParams(collective_id=2, has_side_effects=True),
        name="tail",
    )(g, v, o, *ff)


def place_cols(pieces, me):
    count, (rows, cols) = len(pieces), pieces[0].shape

    def body(me_ref, *refs):
        for r in range(count):
            spot = pl.multiple_of((me_ref[0] ^ r) * cols, cols)
            refs[-1][:, pl.ds(spot, cols)] = refs[r][...]

    return whole_call(
        body, jax.ShapeDtypeStruct((rows, count * cols), pieces[0].dtype), me, *pieces
    )


def take_cols(value, order, groups, me):
    count = len(order)
    rows, cols = value.shape[0], value.shape[1] // count
    each = count // groups

    def body(me_ref, src, *outs):
        for k, r in enumerate(order):
            spot = pl.multiple_of((me_ref[0] ^ r) * cols, cols)
            base = (k % each) * rows
            outs[k // each][base : base + rows, :] = src[:, pl.ds(spot, cols)]

    return whole_call(
        body, [jax.ShapeDtypeStruct((each * rows, cols), value.dtype)] * groups, me, value
    )


def spread_cols(stacked, order, first, last, sections, me, kind=F32):
    count = len(order)
    rows = stacked.shape[0] // count
    cols = (last - first) // sections
    if cols % LANES:
        blocks = stacked.reshape(count, rows, -1)[:, :, first:last]
        blocks = blocks[jnp.argsort(jnp.array(order) ^ me)].reshape(count, rows, sections, cols)
        return blocks.transpose(1, 2, 0, 3).reshape(rows, -1).astype(kind)

    def body(me_ref, src, out):
        for k, r in enumerate(order):
            here = me_ref[0] ^ r
            for c in range(sections):
                spot = pl.multiple_of((c * count + here) * cols, cols)
                out[:, pl.ds(spot, cols)] = src[
                    k * rows : (k + 1) * rows, first + c * cols : first + (c + 1) * cols
                ].astype(kind)

    return whole_call(
        body, jax.ShapeDtypeStruct((rows, count * sections * cols), kind), me, stacked
    )


def spread_rows(stacked, order, first, last, me):
    count = len(order)
    rows = stacked.shape[0] // count

    def body(me_ref, src, out):
        for k, r in enumerate(order):
            spot = pl.multiple_of((me_ref[0] ^ r) * rows, rows)
            out[pl.ds(spot, rows), :] = src[k * rows : (k + 1) * rows, first:last].astype(F32)

    return whole_call(
        body, jax.ShapeDtypeStruct((count * rows, last - first), F32), me, stacked
    )


def pair_mask(shape, head):
    lane = lax.broadcasted_iota(jnp.int32, shape, 1)
    return (lane >= head * HEAD_DIM) & (lane < (head + 1) * HEAD_DIM)


def dot_nt(a, b):
    return lax.dot_general(a, b, (((1,), (1,)), ((), ())), preferred_element_type=F32)


def dot_nn(a, b):
    return lax.dot_general(a, b, (((1,), (0,)), ((), ())), preferred_element_type=F32)


def dot_tn(a, b):
    return lax.dot_general(a, b, (((0,), (0,)), ((), ())), preferred_element_type=F32)


def row_starts(ends_ref, count, row_at, block):
    row = lax.broadcasted_iota(jnp.int32, (1, block), 1) + row_at
    start = jnp.zeros((1, block), jnp.int32)
    for k in range(count):
        start = jnp.where(row >= ends_ref[k], ends_ref[k], start)
    return start


def start_of(ends_ref, count, row):
    start = jnp.int32(0)
    for k in range(count):
        start = jnp.where(row >= ends_ref[k], ends_ref[k], start)
    return start


def over_tiles(ends_ref, count, row_at, block, span, tile):
    start_row = row_starts(ends_ref, count, row_at, block)
    key = lax.broadcasted_iota(jnp.int32, (span, block), 0)
    apart = (key - lax.broadcasted_iota(jnp.int32, (span, block), 1)).astype(F32)
    last = start_of(ends_ref, count, row_at + block - 1)

    def one(j, _):
        at = pl.multiple_of(j * span, span)
        dist = apart + (at - row_at).astype(F32)
        inner = (at >= last) & (at + span <= row_at)

        @pl.when(inner)
        def _():
            tile(at, dist)

        @pl.when(jnp.logical_not(inner))
        def _():
            tile(at, jnp.where((dist <= 0) & (key + at >= start_row), dist, MASKED))

        return 0

    low = lax.div(start_of(ends_ref, count, row_at), span)
    lax.fori_loop(low, lax.div(row_at + block, span), one, 0)


def pair_slice(p):
    return slice(p * LANES, (p + 1) * LANES)


def attend_body(block, span, pairs, count, ends_ref, slope_ref, q_ref, k_ref, v_ref, o_ref, lse_ref, m_ref, l_ref, acc_ref):
    row_at = pl.program_id(0) * block
    m_ref[...] = jnp.full_like(m_ref, -3e38)
    l_ref[...] = jnp.zeros_like(l_ref)
    acc_ref[...] = jnp.zeros_like(acc_ref)
    heads = []
    for p in range(pairs):
        queries = q_ref[:, pair_slice(p)]
        heads += [jnp.where(pair_mask(queries.shape, h), queries, 0).astype(BF) for h in range(2)]

    def tile(at, dist):
        for p in range(pairs):
            keys = k_ref[pl.ds(at, span), pair_slice(p)]
            values = v_ref[pl.ds(at, span), pair_slice(p)].T
            for side in range(2):
                h, half = 2 * p + side, slice(side * HEAD_DIM, (side + 1) * HEAD_DIM)
                scores = dot_nt(keys, heads[h]) + slope_ref[h] * dist
                old = m_ref[h : h + 1, :]
                new = jnp.maximum(old, jnp.max(scores, axis=0, keepdims=True))
                shrink = jnp.exp(old - new)
                weight = jnp.exp(scores - new)
                m_ref[h : h + 1, :] = new
                l_ref[h : h + 1, :] = l_ref[h : h + 1, :] * shrink + jnp.sum(
                    weight, axis=0, keepdims=True
                )
                acc_ref[p, half] = acc_ref[p, half] * shrink + dot_nn(
                    values[half], weight.astype(BF)
                )

    over_tiles(ends_ref, count, row_at, block, span, tile)
    for p in range(pairs):
        top = acc_ref[p, :HEAD_DIM] / l_ref[2 * p : 2 * p + 1, :]
        bottom = acc_ref[p, HEAD_DIM:] / l_ref[2 * p + 1 : 2 * p + 2, :]
        o_ref[:, pair_slice(p)] = jnp.concatenate([top, bottom], axis=0).T.astype(BF)
    lse_ref[...] = m_ref[...] + jnp.log(l_ref[...])


def attend(qkv, ends, slopes, block, span):
    rows, width = qkv.shape[0], qkv.shape[1] // 3
    pairs = width // LANES
    return pl.pallas_call(
        functools.partial(attend_body, block, span, pairs, ends.shape[0]),
        out_shape=(
            jax.ShapeDtypeStruct((rows, width), BF),
            jax.ShapeDtypeStruct((2 * pairs, rows), F32),
        ),
        grid=(rows // block,),
        in_specs=[
            smem(),
            smem(),
            pl.BlockSpec((block, width), lambda i: (i, 0)),
            pl.BlockSpec((rows, width), lambda i: (0, 1)),
            pl.BlockSpec((rows, width), lambda i: (0, 2)),
        ],
        out_specs=(
            pl.BlockSpec((block, width), lambda i: (i, 0)),
            pl.BlockSpec((2 * pairs, block), lambda i: (0, i)),
        ),
        scratch_shapes=[
            pltpu.VMEM((2 * pairs, block), F32),
            pltpu.VMEM((2 * pairs, block), F32),
            pltpu.VMEM((pairs, LANES, block), F32),
        ],
        cost_estimate=pl.CostEstimate(
            flops=4 * rows * rows * width, bytes_accessed=10 * rows * width, transcendentals=rows * rows
        ),
        name="attend",
    )(ends, slopes, qkv, qkv, qkv)


def attend_back_body(
    block, span, pairs, count, ends_ref, slope_ref, lse_ref, q_ref, k_ref, v_ref, o_ref, g_ref, d_ref, dq_acc, dk_acc, dv_acc
):
    row_at = pl.multiple_of(pl.program_id(0) * block, block)
    width = pairs * LANES

    @pl.when(pl.program_id(0) == 0)
    def _():
        dk_acc[...] = jnp.zeros_like(dk_acc)
        dv_acc[...] = jnp.zeros_like(dv_acc)

    dq_acc[...] = jnp.zeros_like(dq_acc)
    q_heads, g_heads, dots = [], [], []
    for p in range(pairs):
        queries, grads = q_ref[:, pair_slice(p)], g_ref[:, pair_slice(p)]
        product = (o_ref[:, pair_slice(p)].astype(F32) * grads.astype(F32)).T
        for side in range(2):
            mask = pair_mask(queries.shape, side)
            half = slice(side * HEAD_DIM, (side + 1) * HEAD_DIM)
            q_heads.append(jnp.where(mask, queries, 0).astype(BF))
            g_heads.append(jnp.where(mask, grads, 0).astype(BF))
            dots.append(jnp.sum(product[half], axis=0, keepdims=True))

    def tile(at, dist):
        for p in range(pairs):
            keys = k_ref[pl.ds(at, span), pair_slice(p)]
            values = v_ref[pl.ds(at, span), pair_slice(p)]
            turned = keys.T
            dv, dk = [], []
            for side in range(2):
                h = 2 * p + side
                scores = dot_nt(keys, q_heads[h]) + slope_ref[h] * dist
                prob = jnp.exp(scores - lse_ref[h : h + 1, :])
                dscore = (prob * (dot_nt(values, g_heads[h]) - dots[h])).astype(BF)
                dv.append(dot_nn(prob.astype(BF), g_heads[h]))
                dk.append(dot_nn(dscore, q_heads[h]))
                rows = slice(h * HEAD_DIM, (h + 1) * HEAD_DIM)
                half = slice(side * HEAD_DIM, (side + 1) * HEAD_DIM)
                dq_acc[rows] += dot_nn(turned[half], dscore)
            dv_acc[pl.ds(at, span), pair_slice(p)] += dv[0] + dv[1]
            dk_acc[pl.ds(at, span), pair_slice(p)] += dk[0] + dk[1]

    over_tiles(ends_ref, count, row_at, block, span, tile)
    d_ref[pl.ds(row_at, block), 0:width] = (dq_acc[...].T * (1.0 / math.sqrt(HEAD_DIM))).astype(BF)

    @pl.when(pl.program_id(0) == pl.num_programs(0) - 1)
    def _():
        d_ref[:, width : 2 * width] = dk_acc[...].astype(BF)
        d_ref[:, 2 * width :] = dv_acc[...].astype(BF)


def attend_back(qkv, out, grad, lse, ends, slopes, block, span):
    rows, width = qkv.shape[0], qkv.shape[1] // 3
    pairs = width // LANES
    return pl.pallas_call(
        functools.partial(attend_back_body, block, span, pairs, ends.shape[0]),
        out_shape=jax.ShapeDtypeStruct((rows, 3 * width), BF),
        grid=(rows // block,),
        in_specs=[
            smem(),
            smem(),
            pl.BlockSpec((2 * pairs, block), lambda i: (0, i)),
            pl.BlockSpec((block, width), lambda i: (i, 0)),
            pl.BlockSpec((rows, width), lambda i: (0, 1)),
            pl.BlockSpec((rows, width), lambda i: (0, 2)),
            pl.BlockSpec((block, width), lambda i: (i, 0)),
            pl.BlockSpec((block, width), lambda i: (i, 0)),
        ],
        out_specs=pl.BlockSpec((rows, 3 * width), lambda i: (0, 0)),
        scratch_shapes=[
            pltpu.VMEM((width, block), F32),
            pltpu.VMEM((rows, width), F32),
            pltpu.VMEM((rows, width), F32),
        ],
        cost_estimate=pl.CostEstimate(
            flops=10 * rows * rows * width, bytes_accessed=20 * rows * width, transcendentals=rows * rows
        ),
        name="attend_back",
    )(ends, slopes, lse, qkv, qkv, qkv, out, grad)


def normalize(values):
    average = jnp.mean(values, axis=-1, keepdims=True)
    centered = values - average
    variance = jnp.mean(centered * centered, axis=-1, keepdims=True)
    scale = lax.rsqrt(variance + 1e-05)
    return centered * scale, scale


def norm_back(grad, gain, normed, scale):
    e = grad * gain
    return scale * (
        e
        - jnp.mean(e, axis=-1, keepdims=True)
        - normed * jnp.mean(e * normed, axis=-1, keepdims=True)
    )


def gelu_and_slope(v):
    c = math.sqrt(2 / math.pi)
    t = jnp.tanh(c * (v + 0.044715 * v * v * v))
    slope = 0.5 * (1 + t) + 0.5 * v * (1 - t * t) * c * (1 + 3 * 0.044715 * v * v)
    return 0.5 * v * (1 + t), slope


def mm(a, b):
    return jnp.dot(a, b, preferred_element_type=F32)


def mm_nt(a, b):
    return lax.dot_general(a, b, (((1,), (1,)), ((), ())), preferred_element_type=F32)


def mm_tn(a, b):
    return lax.dot_general(a, b, (((0,), (0,)), ((), ())), preferred_element_type=F32)


def shards(
    nf,
    ns,
    tokens,
    cotangent,
    seq_lengths,
    stream_order,
    first_gain,
    first_shift,
    qkv_weight,
    query_bias,
    value_bias,
    out_weight,
    out_bias,
    second_gain,
    second_shift,
    up_weight,
    up_bias,
    down_weight,
    down_bias,
):
    f, s = lax.axis_index("fsdp"), lax.axis_index("seq")
    toks, width = tokens.shape
    group = toks * ns
    dl, hl = width // nf, width // ns
    ff = up_weight.shape[1]
    ffl = ff // nf
    q = ffl // ns
    ffs = nf * q
    wide = 3 * hl
    bits_s = falling(ns)
    s_order = order_of(bits_s)
    back = lambda bits: tuple(reversed(bits))

    vectors = jnp.concatenate(
        [first_gain, first_shift, query_bias, value_bias, out_bias, second_gain, second_shift, down_bias, up_bias]
    )
    vec_rows = vectors.shape[0] // wide
    extra = 16
    qkv_shard = jnp.concatenate(
        [lax.dynamic_slice(qkv_weight, (0, k * width + s * hl), (dl, hl)) for k in range(3)], axis=1
    )
    vec_shard = jnp.pad(vectors.reshape(vec_rows, wide), ((0, extra - vec_rows), (0, 0)))
    out_shard = lax.dynamic_slice(out_weight, (0, s * hl), (dl, hl))
    qkv_full, out_cols, vec_all, x_all = head(nf, ns, s_order, qkv_shard, out_shard, vec_shard, tokens)
    up_shard = lax.dynamic_index_in_dim(
        up_weight.reshape(dl, nf, ns, q), s, 2, keepdims=False
    ).reshape(dl, ffs)
    down_shard = lax.dynamic_slice(down_weight, (s * q, 0), (q, width))
    merged = q == dl and q % LANES == 0

    if merged:
        packed = jnp.concatenate([up_shard, down_shard], axis=1)
        packed, cotangent, qkv_full = lax.optimization_barrier((packed, cotangent, qkv_full))
        packed = lax.all_gather(packed, "fsdp", axis=0, tiled=True)
        up_full, down_full = packed[:, :ffs], packed[:, ffs:]
    else:
        up_shard, down_shard, cotangent, qkv_full = lax.optimization_barrier(
            (up_shard, down_shard, cotangent, qkv_full)
        )
        up_full = lax.all_gather(up_shard, "fsdp", axis=0, tiled=True)
        down_full = lax.all_gather(down_shard, "fsdp", axis=0, tiled=True)
    near = bits_s[-1:]
    far = bits_s[:-1]
    out_full = spread_cols(gather_rows(out_cols, "seq", ns, bits_s), s_order, 0, hl, 1, s, BF)
    ct_near = gather_rows(cotangent, "seq", ns, near)
    ct_far = gather_rows(cotangent, "seq", ns, far)[toks:]
    ct_far = gather_rows(ct_far, "seq", ns, near)

    vecs = vec_all.reshape(nf, extra, wide)[:, :vec_rows].reshape(nf, -1, dl).astype(F32)
    full = vecs[:, :8].transpose(1, 0, 2).reshape(8, width)
    gain_one, shift_one, bias_query, bias_value, bias_out, gain_two, shift_two, bias_down = full
    bias_up = lax.dynamic_index_in_dim(vecs[:, 8:].reshape(nf, ns, q), s, 1, keepdims=False)
    bias_up = bias_up.reshape(ffs)
    bias_qkv = jnp.concatenate(
        [
            lax.dynamic_slice(bias_query, (s * hl,), (hl,)),
            jnp.zeros((hl,), F32),
            lax.dynamic_slice(bias_value, (s * hl,), (hl,)),
        ]
    )
    query_scale = jnp.where(jnp.arange(wide) < hl, 1.0 / math.sqrt(HEAD_DIM), 1.0)

    positions = stream_order[0].reshape(ns, toks)[jnp.array(s_order) ^ s].reshape(group)
    ends = jnp.cumsum(seq_lengths[0])
    line = jnp.arange(group)
    block, span = min(512, group), min(512, group)
    ends = ends.astype(jnp.int32)
    heads_here = hl // HEAD_DIM
    slopes = jnp.exp2(
        -(s * heads_here + 1 + jnp.arange(heads_here)).astype(F32) * (8.0 / HEADS)
    )
    to_sorted = (positions[None, :] == line[:, None]).astype(BF)

    n_all, _ = normalize(x_all.astype(F32))
    a_all = (n_all * gain_one + shift_one).astype(BF)
    qkv = ((mm(a_all, qkv_full) + bias_qkv).astype(BF).astype(F32) * query_scale).astype(BF)
    qkv_sorted = mm(to_sorted, qkv).astype(BF)
    o_sorted, lse = attend(qkv_sorted, ends, slopes, block, span)
    o_sorted, ct_near, ct_far, out_full = lax.optimization_barrier((o_sorted, ct_near, ct_far, out_full))
    context_heads = mm_tn(to_sorted, o_sorted).astype(BF)

    def exchange(blocks):
        return [blocks[0]] + [swap(blocks[r], "seq", ns, r) for r in range(1, ns)]

    context = place_cols(
        exchange([context_heads[k * toks : (k + 1) * toks] for k in (s_order.index(r) for r in range(ns))]), s
    )

    x_own = tokens.astype(F32)
    residual = x_own + mm(context, out_full) + bias_out
    n_two, scale_two = normalize(residual)
    m_low = (n_two * gain_two + shift_two).astype(BF)
    m_far = gather_rows(m_low, "seq", ns, far)[toks:]
    m_near = gather_rows(m_low, "seq", ns, near)
    m_far = gather_rows(m_far, "seq", ns, near)

    def feed_forward(m, ct):
        activated, slope = gelu_and_slope(mm(m, up_full) + bias_up)
        act = activated.astype(BF)
        d_pre = (mm_nt(ct, down_full) * slope).astype(BF)
        return act, d_pre, mm_nt(d_pre, up_full).astype(BF)

    act_near, d_pre_near, d_m_near = feed_forward(m_near, ct_near)
    act_far, d_pre_far, d_m_far = feed_forward(m_far, ct_far)

    def home_near(near_part, far_part):
        half = far_part.shape[0] // 2
        keep_near = near_part[:toks].astype(F32) + swap(near_part[toks:], "seq", ns, near[0]).astype(F32)
        keep_far = far_part[:half].astype(F32) + swap(far_part[half:], "seq", ns, near[0]).astype(F32)
        return keep_near, keep_far.astype(BF)

    def home_far(keep_near, keep_far):
        blocks = dict(zip(order_of(far)[1:], jnp.split(keep_far, ns // 2 - 1)))
        blocks[0] = keep_near
        for bit in back(far):
            for r in sorted(blocks):
                if r & bit:
                    arrived = swap(blocks.pop(r).astype(BF), "seq", ns, bit)
                    blocks[r ^ bit] = blocks[r ^ bit].astype(F32) + arrived.astype(F32)
        return blocks[0]

    kept, act_near, act_far, d_pre_near, d_pre_far = lax.optimization_barrier(
        (home_near(d_m_near, d_m_far), act_near, act_far, d_pre_near, d_pre_far)
    )
    d_m = home_far(*kept)
    total_near, total_far = home_near(mm(act_near, down_full).astype(BF), mm(act_far, down_full).astype(BF))
    grad_up = (mm_tn(m_near, d_pre_near) + mm_tn(m_far, d_pre_far)).astype(BF)
    grad_down = (mm_tn(act_near, ct_near) + mm_tn(act_far, ct_far)).astype(BF)
    grad_up_bias = jnp.sum(d_pre_near, axis=0, dtype=F32) + jnp.sum(d_pre_far, axis=0, dtype=F32)

    def scatter_whole(value):
        return lax.psum_scatter(value, "fsdp", scatter_dimension=0, tiled=True)

    if merged:
        grad_ff = [scatter_whole(jnp.concatenate([grad_up, grad_down], axis=1))]
    else:
        grad_ff = []
        grad_up = gather_rows(scatter_whole(grad_up), "seq", ns, bits_s)
        grad_down = gather_rows(scatter_whole(grad_down), "seq", ns, bits_s)
        up_all = spread_cols(grad_up, s_order, 0, ffs, nf, s)
        down_all = spread_rows(grad_down, s_order, 0, width, s)

    ct_own = cotangent.astype(F32)
    grad_down_bias = jnp.sum(ct_own, axis=0)
    grad_gain_two = jnp.sum(d_m * n_two, axis=0)
    grad_shift_two = jnp.sum(d_m, axis=0)
    d_res = ct_own + norm_back(d_m, gain_two, n_two, scale_two)
    d_att = d_res.astype(BF)
    grad_out_bias = jnp.sum(d_att, axis=0, dtype=F32)
    d_context = exchange(take_cols(mm_nt(d_att, out_full).astype(BF), list(range(ns)), ns, s))
    d_context = jnp.concatenate([d_context[r] for r in s_order], axis=0)
    total_near, total_far, d_context = lax.optimization_barrier((total_near, total_far, d_context))
    output = (residual + home_far(total_near, total_far) + bias_down).astype(BF)
    d_o_sorted = mm(to_sorted, d_context).astype(BF)
    grad_out = take_cols(mm_tn(context, d_att).astype(BF), s_order, 2, s)
    grad_out = scatter_rows(*grad_out, "seq", ns, back(bits_s), BF)

    d_qkv_sorted = attend_back(
        qkv_sorted, o_sorted, d_o_sorted, lse, ends, slopes, block, span // 2
    )
    d_qkv_sorted, output, grad_out = lax.optimization_barrier((d_qkv_sorted, output, grad_out))
    d_qkv = mm_tn(to_sorted, d_qkv_sorted).astype(BF)
    d_a_part = mm_nt(d_qkv, qkv_full)
    d_a_low = d_a_part.astype(BF)
    d_a_own, d_a = scatter_rows(d_a_low[: group // 2], d_a_low[group // 2 :], "seq", ns, back(bits_s), None)
    grad_qkv = mm_tn(a_all, d_qkv).astype(BF)
    grad_bias_qkv = jnp.sum(d_qkv, axis=0, dtype=F32)
    grad_gain_one = jnp.sum(d_a_part * n_all, axis=0)
    grad_shift_one = jnp.sum(d_a_part, axis=0)
    n_own, scale_own = normalize(x_own)

    def spread(part):
        return lax.dynamic_update_slice(jnp.zeros((width,), F32), part, (s * hl,))

    vec_part = jnp.stack(
        [
            grad_gain_one,
            grad_shift_one,
            spread(grad_bias_qkv[:hl]),
            spread(grad_bias_qkv[2 * hl :]),
            grad_out_bias,
            grad_gain_two,
            grad_shift_two,
            grad_down_bias,
        ]
    )
    vec_part = vec_part.reshape(8, nf, dl).transpose(1, 0, 2)
    up_part = lax.dynamic_update_slice(
        jnp.zeros((nf, ns, q), F32), grad_up_bias.reshape(nf, 1, q), (0, s, 0)
    ).reshape(nf, -1, dl)
    vec_part = jnp.concatenate([vec_part, up_part], axis=1).reshape(nf, vec_rows, wide)
    vec_part = jnp.pad(vec_part, ((0, 0), (0, extra - vec_rows), (0, 0))).astype(BF)
    vec_part = vec_part.reshape(nf * extra, wide)
    qkv_all, vec_sum, out_all, *ff_all = tail_call(nf, ns, grad_qkv, vec_part, grad_out, *grad_ff)
    if merged:
        up_all, down_all = ff_all
    d_a, vec_sum = lax.optimization_barrier((d_a, vec_sum))
    d_a = d_a_own.astype(F32) + d_a.astype(F32)
    tokens_grad = d_res + norm_back(d_a, gain_one, n_own, scale_own)
    vec_sum = vec_sum[:vec_rows].reshape(-1, dl)
    return (
        output,
        tokens_grad,
        vec_sum[0],
        vec_sum[1],
        qkv_all,
        vec_sum[2],
        vec_sum[3],
        out_all,
        vec_sum[4],
        vec_sum[5],
        vec_sum[6],
        up_all,
        vec_sum[8:].reshape(ffl),
        down_all,
        vec_sum[7],
    )


def solution(mesh):
    rows, cols, vec = P(("fsdp", "seq"), None), P("fsdp", None), P("fsdp")
    return jax.shard_map(
        functools.partial(shards, mesh.shape["fsdp"], mesh.shape["seq"]),
        mesh=mesh,
        in_specs=(rows, rows, cols, cols, vec, vec, cols, vec, vec, cols, vec, vec, vec, cols, vec, cols, vec),
        out_specs=(rows, rows, vec, vec, cols, vec, vec, cols, vec, vec, vec, cols, vec, cols, vec),
        check_vma=False,
    )
```
